32 devices in a mesh: dp: 8 (over z, y), mp: 4 (over x, core).
Axes of the slice: x: 2, y: 2, z: 4, core: 2. Of those that a mesh axis runs over, the one named last changes fastest.
Arguments:
- wide_state: bfloat16 [16, 2, 768, 1024], P('dp', None, 'mp'), may hold values from -6 to 6
- encoder: bfloat16 [16, 512, 768], P('dp', 'mp'), may hold values from -6 to 6
- segments: int32 [16, 1024], P('dp'), may hold values from 0 to 15, never falling along the last dimension, each value on 1 to 512 neighbouring positions
- key_valid: int32 [16, 1024], P('dp'), may hold values from 0 to 1, as said below
- self_qkv: bfloat16 [3, 768, 768], P(None, 'mp'), may hold values from -0.21875 to 0.21875
- self_out: bfloat16 [768, 768], P('mp'), may hold values from -0.875 to 0.875
- cross_qkv: bfloat16 [3, 768, 768], P(None, 'mp'), may hold values from -0.21875 to 0.21875
- cross_out: bfloat16 [768, 768], P('mp'), may hold values from -0.625 to 0.625
- ffn_in: bfloat16 [2, 768, 3072], P(None, None, 'mp'), may hold values from -0.21875 to 0.21875
- ffn_out: bfloat16 [3072, 768], P('mp'), may hold values from -0.109375 to 0.109375
- norm_gains: float32 [3, 768], replicated, may hold values from 0.5 to 1.5
- predict: float32 [2, 2], replicated, may hold values from 0.1 to 1.9
- correct: float32 [2], replicated, may hold values from 0.1 to 1.9
- cotangent: bfloat16 [16, 2, 768, 1024], P('dp', None, 'mp'), may hold values from -6 to 6
Outputs:
- new_state: bfloat16 [16, 2, 768, 1024], P('dp', None, 'mp')
- grad_state: float32 [16, 2, 768, 1024], P('dp', None, 'mp')
- grad_encoder: float32 [16, 512, 768], P('dp', 'mp')
- grad_self_qkv: float32 [3, 768, 768], P(None, 'mp', 'dp')
- grad_self_out: float32 [768, 768], P('mp', 'dp')
- grad_cross_qkv: float32 [3, 768, 768], P(None, 'mp', 'dp')
- grad_cross_out: float32 [768, 768], P('mp', 'dp')
- grad_ffn_in: float32 [2, 768, 3072], P(None, 'dp', 'mp')
- grad_ffn_out: float32 [3072, 768], P('mp', 'dp')
- grad_norm_gains: float32 [3, 768], replicated
- grad_predict: float32 [2, 2], replicated
- grad_correct: float32 [2], replicated
The draws below stay inside these ranges and needn't reach their ends.
Inputs may be any that keep to these rules, and one draw needn't show every extreme that they name: `segments`: within a row the numbers never fall; a document spans 1 to 512 positions. `key_valid`: in each row the ones come first, followed by 1 to 256 zeros.
All inputs are finite; a program needn't handle non-finite values.
Results may differ from the reference program's by a relative error of at most 0.02.
Values may be sent and summed in bfloat16 or wider, within the bound.
A program may use at most 256 MiB of HBM per device.

```python
import math
import jax
import jax.numpy as jnp
import numpy as np
from jax import lax

D = 768
HEADS = 12
HEAD = 64
FF = 3072
K = 2
LENGTH = 1024
ENC = 512
ROWS_DEV = 2
ROWS = 16


def draw_key_valid(key, part):
    padding = jax.random.randint(key, (ROWS, 1), 1, LENGTH // 4 + 1)
    position = jnp.arange(LENGTH, dtype=jnp.int32)[None, :]
    return (position < LENGTH - padding).astype(jnp.int32)


def steps_of(key, extent, split, least, top_value):
    loudness = 1.0
    for dim, blocks in split:
        draws = jax.random.uniform(jax.random.fold_in(jax.random.fold_in(key, 6), dim), (blocks,), jnp.float32, least / len(split), top_value / len(split))
        loudness = loudness * jnp.repeat(jnp.exp(draws), extent[dim] // blocks).reshape((-1,) + (1,) * (len(extent) - 1 - dim))
    return loudness


def profile(amount, total, reach, skew):
    portions = [(1 << 20) // math.isqrt(rank ** skew) + 1 for rank in range(2, amount + 1)]
    surplus, given = total - reach - (amount - 1), [1] * (amount - 1)
    while surplus > 0:
        candidates = [i for i in range(amount - 1) if given[i] < reach]
        pool, remaining = sum([portions[i] for i in candidates]), surplus
        for i in candidates:
            extra = min(reach - given[i], max(1, remaining * portions[i] // pool), surplus)
            given[i] = given[i] + extra
            surplus = surplus - extra
    return np.array([reach] + given)


def ragged_sizes(stream_key, amount, total, bound, slope):
    if amount == 2:
        one = jax.random.randint(stream_key, (), max(1, total - bound), min(bound, total - 1) + 1)
        return jnp.stack([one, total - one])
    tallies = jnp.asarray(profile(amount, total, bound, slope), jnp.int32)
    pairs = (amount - 1) // 2
    donor, receiver = tallies[1:1 + 2 * pairs:2], tallies[2:2 + 2 * pairs:2]
    slack = jnp.minimum(donor - 1, bound - receiver)
    shifted = jax.random.randint(jax.random.fold_in(stream_key, 1), (pairs,), 0, 1 << 20) % (slack + 1)
    tallies = tallies.at[1:1 + 2 * pairs:2].set(donor - shifted).at[2:2 + 2 * pairs:2].set(receiver + shifted)
    return tallies[jax.random.permutation(jax.random.fold_in(stream_key, 2), amount)]


def centred(key, shape, spread, bound, cuts=(), kind=jnp.bfloat16):
    values = spread * jax.random.normal(key, shape, jnp.float32)
    if cuts:
        values = values * steps_of(key, shape, cuts, -0.22, 0.18)
    return jnp.clip(values, -bound, bound).astype(kind)


def setup_inputs(seed: int = 0) -> dict:
    seeds = jax.random.split(jax.random.key(seed), 15)
    wide_state = centred(seeds[0], (ROWS, K, D, LENGTH), 1.0, 6.0, ((0, 8), (2, 4)))
    encoder = centred(seeds[1], (ROWS, ENC, D), 1.0, 6.0, ((0, 8), (1, 4)))
    segments = jax.vmap(lambda own: jnp.searchsorted(jnp.cumsum(ragged_sizes(own, max(LENGTH // 64, 4), LENGTH, LENGTH // 2, 2)), jnp.arange(LENGTH), side="right"))(jax.random.split(seeds[2], ROWS)).reshape((ROWS, LENGTH)).astype(jnp.int32)
    key_valid = draw_key_valid(jax.random.fold_in(seeds[14], 71), 0)
    self_qkv = centred(seeds[4], (3, D, D), D ** -0.5, 0.21875, ((1, 4),))
    self_out = centred(seeds[5], (D, D), (D // 16) ** -0.5, 0.875, ((0, 4),))
    cross_qkv = centred(seeds[6], (3, D, D), D ** -0.5, 0.21875, ((1, 4),))
    cross_out = centred(seeds[7], (D, D), (D // 8) ** -0.5, 0.625, ((0, 4),))
    ffn_in = centred(seeds[8], (2, D, FF), D ** -0.5, 0.21875, ((2, 4),))
    ffn_out = centred(seeds[9], (FF, D), FF ** -0.5, 0.109375, ((0, 4),))
    norm_gains = jnp.clip(1.0 + 0.1 * jax.random.normal(seeds[10], (3, D), jnp.float32), 0.5, 1.5)
    predict = jnp.clip(1.0 + 0.18 * jax.random.normal(seeds[11], (K, K), jnp.float32), 0.1, 1.9)
    correct = jnp.clip(1.0 + 0.18 * jax.random.normal(seeds[12], (K,), jnp.float32), 0.1, 1.9)
    cotangent = centred(seeds[13], (ROWS, K, D, LENGTH), 1.0, 6.0, ((0, 8), (2, 4)))
    return {"wide_state": wide_state, "encoder": encoder, "segments": segments, "key_valid": key_valid, "self_qkv": self_qkv, "self_out": self_out, "cross_qkv": cross_qkv, "cross_out": cross_out, "ffn_in": ffn_in, "ffn_out": ffn_out, "norm_gains": norm_gains, "predict": predict, "correct": correct, "cotangent": cotangent}


EPSILON = 1e-06
MASKED_SCORE = -1e+30

@jax.custom_vjp
def low(v):
    return lax.optimization_barrier(v.astype(jnp.bfloat16)).astype(jnp.float32)

@jax.custom_vjp
def low_back(v):
    return v

def low_keep(v):
    return (low(v), None)

def low_pass(kept, grad):
    return (grad,)

def back_keep(v):
    return (v, None)

def back_low(kept, grad):
    return (low(grad),)
low.defvjp(low_keep, low_pass)
low_back.defvjp(back_keep, back_low)

def rms_norm(values, norm_gain):
    mean_sq = lax.optimization_barrier(jnp.mean(values * values, axis=-1, keepdims=True))
    return values * lax.rsqrt(mean_sq + EPSILON) * norm_gain

def product(left_side, right_side, pattern):
    return jnp.einsum(pattern, left_side, right_side, precision=lax.Precision.HIGHEST)

def gated_unit(gate_pre, up_pre):
    return jax.nn.gelu(gate_pre, approximate=True) * up_pre

def self_mask(segments, key_valid):
    position = jnp.arange(segments.shape[1], dtype=jnp.int32)
    earlier = position[None, None, :] <= position[None, :, None]
    itself = position[None, None, :] == position[None, :, None]
    same_doc = segments[:, :, None] == segments[:, None, :]
    return same_doc & earlier & (key_valid[:, None, :] > 0) | itself

def attention(queries, key_rows, value_rows, allowed):
    q_heads = queries.reshape(queries.shape[0], queries.shape[1], HEADS, HEAD)
    k_heads = key_rows.reshape(key_rows.shape[0], key_rows.shape[1], HEADS, HEAD)
    v_heads = value_rows.reshape(value_rows.shape[0], value_rows.shape[1], HEADS, HEAD)
    scores = low_back(product(q_heads, k_heads, 'rqhd,rkhd->rhqk') * HEAD ** (-0.5))
    if allowed is not None:
        scores = jnp.where(allowed[:, None], scores, MASKED_SCORE)
    attn_probs = low(jax.nn.softmax(scores, axis=-1))
    mixed_heads = product(attn_probs, v_heads, 'rhqk,rkhd->rqhd')
    return low_back(low(mixed_heads.reshape(queries.shape)))

def group_layer(weights, pieces):
    self_qkv, self_out, cross_qkv, cross_out, ffn_in, ffn_out, norm_gains, predict, correct = weights
    state_g, encoder_g, segments_g, valid_g = pieces
    block_a = state_g[:, :, 0]
    block_b = state_g[:, :, 1]
    guess_a = predict[0, 0] * block_a + predict[0, 1] * block_b
    guess_b = predict[1, 0] * block_a + predict[1, 1] * block_b
    active = low_back(low(guess_a))
    normed_a = low(rms_norm(active, norm_gains[0]))
    queries = low_back(low(product(normed_a, self_qkv[0], 'rtd,de->rte')))
    key_rows = low_back(low(product(normed_a, self_qkv[1], 'rtd,de->rte')))
    value_rows = low_back(low(product(normed_a, self_qkv[2], 'rtd,de->rte')))
    self_mix = attention(queries, key_rows, value_rows, self_mask(segments_g, valid_g))
    attn_out = low_back(product(self_mix, self_out, 'rtd,de->rte'))
    resid_b = active + attn_out
    normed_b = low(rms_norm(resid_b, norm_gains[1]))
    cross_q = low_back(low(product(normed_b, cross_qkv[0], 'rtd,de->rte')))
    cross_k = low_back(low(product(encoder_g, cross_qkv[1], 'rsd,de->rse')))
    cross_v = low_back(low(product(encoder_g, cross_qkv[2], 'rsd,de->rse')))
    cross_mix = attention(cross_q, cross_k, cross_v, None)
    cross_res = low_back(product(cross_mix, cross_out, 'rtd,de->rte'))
    resid_c = resid_b + cross_res
    normed_c = low(rms_norm(resid_c, norm_gains[2]))
    gate_pre = low_back(product(normed_c, ffn_in[0], 'rtd,df->rtf'))
    up_pre = low_back(product(normed_c, ffn_in[1], 'rtd,df->rtf'))
    hidden = low(gated_unit(gate_pre, up_pre))
    ffn_res = low_back(product(hidden, ffn_out, 'rtf,fd->rtd'))
    branch = low_back(low(attn_out + cross_res))
    branch_sum = branch + ffn_res
    return jnp.stack([guess_a + correct[0] * branch_sum, guess_b + correct[1] * branch_sum], axis=2)

def reference(wide_state, encoder, segments, key_valid, self_qkv, self_out, cross_qkv, cross_out, ffn_in, ffn_out, norm_gains, predict, correct, cotangent):
    groups = wide_state.shape[0] // ROWS_DEV

    def grouped(whole_array):
        return whole_array.reshape((groups, ROWS_DEV) + whole_array.shape[1:])

    def forward(state_f, encoder_f, sqkv, sout, cqkv, cout, fin, fout, gains_f, predict_f, correct_f):
        weights = (sqkv, sout, cqkv, cout, fin, fout, gains_f, predict_f, correct_f)
        layer_step = jax.checkpoint(group_layer)

        def one_group(pieces):
            return layer_step(weights, pieces)
        result = lax.map(one_group, (grouped(state_f), grouped(encoder_f), grouped(segments), grouped(key_valid)))
        return result.reshape(state_f.shape)
    state_rows = jnp.transpose(wide_state.astype(jnp.float32), (0, 3, 1, 2))
    new_state, pullback = jax.vjp(forward, state_rows, encoder.astype(jnp.float32), self_qkv.astype(jnp.float32), self_out.astype(jnp.float32), cross_qkv.astype(jnp.float32), cross_out.astype(jnp.float32), ffn_in.astype(jnp.float32), ffn_out.astype(jnp.float32), norm_gains, predict, correct)
    cot_rows = jnp.transpose(cotangent.astype(jnp.float32), (0, 3, 1, 2))
    gradients = pullback(cot_rows)
    new_out = jnp.transpose(new_state, (0, 2, 3, 1)).astype(jnp.bfloat16)
    grad_out = jnp.transpose(gradients[0], (0, 2, 3, 1))
    return (new_out, grad_out, gradients[1], gradients[2], gradients[3], gradients[4], gradients[5], gradients[6], gradients[7], gradients[8], gradients[9], gradients[10])
```

```python
import functools

import jax
import jax.numpy as jnp
from jax import lax
from jax.experimental import pallas as pl
from jax.experimental.pallas import tpu as pltpu
from jax.sharding import PartitionSpec as P

HEADS = 12
HEAD = 64


EPSILON = 1e-06
MASKED_SCORE = -1e30


def rms_norm(values, norm_gain):
    mean_sq = jnp.mean(values * values, axis=-1, keepdims=True)
    return values * lax.rsqrt(mean_sq + EPSILON) * norm_gain


def rms_back(values, norm_gain, incoming):
    _, pullback = jax.vjp(rms_norm, values, norm_gain)
    return pullback(incoming)


def gated_unit(gate_pre, up_pre):
    return jax.nn.gelu(gate_pre, approximate=True) * up_pre


def head_split(matrix):
    return matrix.reshape(matrix.shape[0], matrix.shape[1], HEADS, HEAD)


def head_join(tensor):
    return tensor.reshape(tensor.shape[0], tensor.shape[1], HEADS * HEAD)


def self_mask(segments, key_valid, query_start, query_len, key_len):
    seg_query = lax.dynamic_slice_in_dim(segments, query_start, query_len, 1)
    live_key = key_valid > 0
    query_pos = query_start + jnp.arange(query_len, dtype=jnp.int32)
    key_pos = jnp.arange(key_len, dtype=jnp.int32)
    earlier = key_pos[None, None, :] <= query_pos[None, :, None]
    itself = key_pos[None, None, :] == query_pos[None, :, None]
    same_doc = seg_query[:, :, None] == segments[:, None, :]
    return same_doc & earlier & live_key[:, None, :] | itself


def scores_of(queries, key_rows, allowed):
    scores = jnp.einsum(
        "rqhd,rkhd->rhqk",
        head_split(queries),
        head_split(key_rows),
        preferred_element_type=jnp.float32,
    ) * HEAD ** (-0.5)
    if allowed is None:
        return scores
    return jnp.where(allowed[:, None], scores, MASKED_SCORE)


def attend(queries, key_rows, value_rows, allowed):
    scores = scores_of(queries, key_rows, allowed)
    top_score = jnp.max(scores, axis=-1, keepdims=True)
    exponent = jnp.exp(scores - top_score)
    row_total = jnp.sum(exponent, axis=-1, keepdims=True)
    attn_probs = (exponent / row_total).astype(jnp.bfloat16)
    mixed_heads = jnp.einsum(
        "rhqk,rkhd->rqhd", attn_probs, head_split(value_rows), preferred_element_type=jnp.float32
    )
    return (head_join(mixed_heads).astype(jnp.bfloat16), top_score + jnp.log(row_total))


def query_side_grads(queries, key_rows, value_rows, allowed, log_total, grad_mix):
    scores = scores_of(queries, key_rows, allowed)
    attn_probs = jnp.exp(scores - log_total)
    grad_heads = head_split(grad_mix)
    grad_probs = jnp.einsum(
        "rqhd,rkhd->rhqk", grad_heads, head_split(value_rows), preferred_element_type=jnp.float32
    )
    row_dot = jnp.sum(grad_probs * attn_probs, axis=-1, keepdims=True)
    grad_scores = (attn_probs * (grad_probs - row_dot)).astype(jnp.bfloat16)
    grad_query = head_join(
        jnp.einsum(
            "rhqk,rkhd->rqhd", grad_scores, head_split(key_rows), preferred_element_type=jnp.float32
        )
    ) * HEAD ** (-0.5)
    grad_key = head_join(
        jnp.einsum(
            "rhqk,rqhd->rkhd", grad_scores, head_split(queries), preferred_element_type=jnp.float32
        )
    ) * HEAD ** (-0.5)
    grad_value = head_join(
        jnp.einsum(
            "rhqk,rqhd->rkhd",
            attn_probs.astype(jnp.bfloat16),
            grad_heads,
            preferred_element_type=jnp.float32,
        )
    )
    return (grad_query, jnp.stack([grad_key, grad_value]), row_dot)


def shards(
    wide_state,
    encoder,
    segments,
    key_valid,
    self_qkv,
    self_out,
    cross_qkv,
    cross_out,
    ffn_in,
    ffn_out,
    norm_gains,
    predict,
    correct,
    cotangent,
):
    length = segments.shape[1]
    local_len = length // lax.axis_size("mp")
    offset = lax.axis_index("mp") * local_len
    state_f = jnp.transpose(wide_state.astype(jnp.float32), (0, 3, 1, 2))
    block_a = state_f[:, :, 0]
    block_b = state_f[:, :, 1]
    guess_a = predict[0, 0] * block_a + predict[0, 1] * block_b
    guess_b = predict[1, 0] * block_a + predict[1, 1] * block_b
    w_self, w_self_out, w_cross, w_cross_out = (
        lax.all_gather(self_qkv, "mp", axis=1, tiled=True),
        lax.all_gather(self_out, "mp", axis=0, tiled=True),
        lax.all_gather(cross_qkv, "mp", axis=1, tiled=True),
        lax.all_gather(cross_out, "mp", axis=0, tiled=True),
    )
    active = lax.all_to_all(
        guess_a.astype(jnp.bfloat16), "mp", split_axis=1, concat_axis=2, tiled=True
    )
    cross_kv = jnp.einsum(
        "rsd,cde->crse", encoder, w_cross[1:], preferred_element_type=jnp.float32
    ).astype(jnp.bfloat16)
    resid_a = active.astype(jnp.float32)
    normed_a = rms_norm(resid_a, norm_gains[0]).astype(jnp.bfloat16)
    self_proj = jnp.einsum(
        "rtd,cde->crte", normed_a, w_self, preferred_element_type=jnp.float32
    ).astype(jnp.bfloat16)
    queries = self_proj[0]
    all_kv, all_ckv = (
        lax.all_gather(self_proj[1:], "mp", axis=2, tiled=True),
        lax.all_gather(cross_kv, "mp", axis=2, tiled=True),
    )
    allowed = self_mask(segments, key_valid, offset, local_len, length)
    self_mix, self_log = attend(queries, all_kv[0], all_kv[1], allowed)
    attn_out = jnp.einsum("rtd,de->rte", self_mix, w_self_out, preferred_element_type=jnp.float32)
    resid_b = resid_a + attn_out
    normed_b = rms_norm(resid_b, norm_gains[1]).astype(jnp.bfloat16)
    cross_q = jnp.einsum(
        "rtd,de->rte", normed_b, w_cross[0], preferred_element_type=jnp.float32
    ).astype(jnp.bfloat16)
    cross_mix, cross_log = attend(cross_q, all_ckv[0], all_ckv[1], None)
    cross_res = jnp.einsum(
        "rtd,de->rte", cross_mix, w_cross_out, preferred_element_type=jnp.float32
    )
    resid_c = resid_b + cross_res
    normed_c = rms_norm(resid_c, norm_gains[2]).astype(jnp.bfloat16)
    all_normed = lax.all_gather(normed_c, "mp", axis=1, tiled=True)
    gate_up = jnp.einsum("rtd,cdf->crtf", all_normed, ffn_in, preferred_element_type=jnp.float32)
    hidden = gated_unit(gate_up[0], gate_up[1]).astype(jnp.bfloat16)
    ffn_part = jnp.einsum("rtf,fd->rtd", hidden, ffn_out, preferred_element_type=jnp.float32)
    ffn_res = lax.psum_scatter(
        ffn_part.astype(jnp.bfloat16), "mp", scatter_dimension=2, tiled=True
    ).astype(jnp.float32)
    branch_rows = (attn_out + cross_res).astype(jnp.bfloat16)
    branch_cols = lax.all_to_all(branch_rows, "mp", split_axis=2, concat_axis=1, tiled=True)
    branch_sum = branch_cols.astype(jnp.float32) + ffn_res
    new_rows = jnp.stack(
        [guess_a + correct[0] * branch_sum, guess_b + correct[1] * branch_sum], axis=2
    )
    new_state = jnp.transpose(new_rows, (0, 2, 3, 1)).astype(jnp.bfloat16)
    cot_f = jnp.transpose(cotangent.astype(jnp.float32), (0, 3, 1, 2))
    cot_a = cot_f[:, :, 0]
    cot_b = cot_f[:, :, 1]
    grad_branch = (correct[0] * cot_a + correct[1] * cot_b).astype(jnp.bfloat16)
    grad_correct = jnp.stack([jnp.sum(cot_a * branch_sum), jnp.sum(cot_b * branch_sum)])
    all_grad = lax.all_gather(grad_branch, "mp", axis=2, tiled=True)
    grad_rows = lax.dynamic_slice_in_dim(all_grad, offset, local_len, 1).astype(jnp.float32)
    grad_hidden = jnp.einsum("rtd,fd->rtf", all_grad, ffn_out, preferred_element_type=jnp.float32)
    grad_ffn_out = jnp.einsum("rtf,rtd->fd", hidden, all_grad, preferred_element_type=jnp.float32)
    _, gate_back = jax.vjp(gated_unit, gate_up[0], gate_up[1])
    grad_gate, grad_up = gate_back(grad_hidden)
    grad_gate_up = jnp.stack([grad_gate, grad_up]).astype(jnp.bfloat16)
    grad_ffn_in = jnp.einsum(
        "rtd,crtf->cdf", all_normed, grad_gate_up, preferred_element_type=jnp.float32
    )
    normed_part = jnp.einsum(
        "crtf,cdf->rtd", grad_gate_up, ffn_in, preferred_element_type=jnp.float32
    )
    grad_normed_c = lax.psum_scatter(normed_part, "mp", scatter_dimension=1, tiled=True)
    grad_resid_c, gain_grad_c = rms_back(resid_c, norm_gains[2], grad_normed_c)
    grad_cross_b = (grad_rows + grad_resid_c).astype(jnp.bfloat16)
    grad_cross_out = jnp.einsum(
        "rtd,rte->de", cross_mix, grad_cross_b, preferred_element_type=jnp.float32
    )
    grad_cross_mix = jnp.einsum(
        "rte,de->rtd", grad_cross_b, w_cross_out, preferred_element_type=jnp.float32
    ).astype(jnp.bfloat16)
    grad_cq, cross_key_part, _ = query_side_grads(
        cross_q, all_ckv[0], all_ckv[1], None, cross_log, grad_cross_mix
    )
    grad_cq_b = grad_cq.astype(jnp.bfloat16)
    grad_cross_first = jnp.einsum(
        "rtd,rte->de", normed_b, grad_cq_b, preferred_element_type=jnp.float32
    )
    grad_normed_b = jnp.einsum(
        "rte,de->rtd", grad_cq_b, w_cross[0], preferred_element_type=jnp.float32
    )
    resid_b_part, gain_grad_b = rms_back(resid_b, norm_gains[1], grad_normed_b)
    grad_resid_b = grad_resid_c + resid_b_part
    grad_attn_b = (grad_rows + grad_resid_b).astype(jnp.bfloat16)
    grad_self_out = jnp.einsum(
        "rtd,rte->de", self_mix, grad_attn_b, preferred_element_type=jnp.float32
    )
    grad_self_mix = jnp.einsum(
        "rte,de->rtd", grad_attn_b, w_self_out, preferred_element_type=jnp.float32
    ).astype(jnp.bfloat16)
    grad_query, self_key_part, _ = query_side_grads(
        queries, all_kv[0], all_kv[1], allowed, self_log, grad_self_mix
    )
    own_kv, own_ckv = (
        lax.psum_scatter(
            self_key_part.astype(jnp.bfloat16), "mp", scatter_dimension=2, tiled=True
        ).astype(jnp.float32),
        lax.psum_scatter(
            cross_key_part.astype(jnp.bfloat16), "mp", scatter_dimension=2, tiled=True
        ).astype(jnp.float32),
    )
    own_kv_b = own_kv.astype(jnp.bfloat16)
    own_ckv_b = own_ckv.astype(jnp.bfloat16)
    grad_qkv_b = jnp.concatenate([grad_query.astype(jnp.bfloat16)[None], own_kv_b], axis=0)
    grad_self_qkv = jnp.einsum(
        "rtd,crte->cde", normed_a, grad_qkv_b, preferred_element_type=jnp.float32
    )
    grad_normed_a = jnp.einsum(
        "crte,cde->rtd", grad_qkv_b, w_self, preferred_element_type=jnp.float32
    )
    grad_cross_kv = jnp.einsum(
        "rsd,crse->cde", encoder, own_ckv_b, preferred_element_type=jnp.float32
    )
    grad_encoder = jnp.einsum(
        "crse,cde->rsd", own_ckv_b, w_cross[1:], preferred_element_type=jnp.float32
    )
    grad_cross_qkv = jnp.concatenate([grad_cross_first[None], grad_cross_kv], axis=0)
    resid_a_part, gain_grad_a = rms_back(resid_a, norm_gains[0], grad_normed_a)
    grad_active = (grad_resid_b + resid_a_part).astype(jnp.bfloat16)
    grad_cols = lax.all_to_all(grad_active, "mp", split_axis=2, concat_axis=1, tiled=True).astype(
        jnp.float32
    )
    grad_guess_a = cot_a + grad_cols
    grad_predict = jnp.stack(
        [
            jnp.stack([jnp.sum(grad_guess_a * block_a), jnp.sum(grad_guess_a * block_b)]),
            jnp.stack([jnp.sum(cot_b * block_a), jnp.sum(cot_b * block_b)]),
        ]
    )
    grad_rows_state = jnp.stack(
        [
            predict[0, 0] * grad_guess_a + predict[1, 0] * cot_b,
            predict[0, 1] * grad_guess_a + predict[1, 1] * cot_b,
        ],
        axis=2,
    )
    grad_state = jnp.transpose(grad_rows_state, (0, 2, 3, 1))
    gain_grads = jnp.stack([gain_grad_a, gain_grad_b, gain_grad_c])
    part_self_qkv, part_self_out, part_cross_qkv, part_cross_out, part_ffn_in, part_ffn_out = (
        lax.psum_scatter(
            grad_self_qkv.astype(jnp.bfloat16), "dp", scatter_dimension=2, tiled=True
        ).astype(jnp.float32),
        lax.psum_scatter(
            grad_self_out.astype(jnp.bfloat16), "dp", scatter_dimension=1, tiled=True
        ).astype(jnp.float32),
        lax.psum_scatter(
            grad_cross_qkv.astype(jnp.bfloat16), "dp", scatter_dimension=2, tiled=True
        ).astype(jnp.float32),
        lax.psum_scatter(
            grad_cross_out.astype(jnp.bfloat16), "dp", scatter_dimension=1, tiled=True
        ).astype(jnp.float32),
        lax.psum_scatter(
            grad_ffn_in.astype(jnp.bfloat16), "dp", scatter_dimension=1, tiled=True
        ).astype(jnp.float32),
        lax.psum_scatter(
            grad_ffn_out.astype(jnp.bfloat16), "dp", scatter_dimension=1, tiled=True
        ).astype(jnp.float32),
    )
    final_self_qkv, final_self_out, final_cross_qkv, final_cross_out = (
        lax.psum_scatter(
            part_self_qkv.astype(jnp.bfloat16), "mp", scatter_dimension=1, tiled=True
        ).astype(jnp.float32),
        lax.psum_scatter(
            part_self_out.astype(jnp.bfloat16), "mp", scatter_dimension=0, tiled=True
        ).astype(jnp.float32),
        lax.psum_scatter(
            part_cross_qkv.astype(jnp.bfloat16), "mp", scatter_dimension=1, tiled=True
        ).astype(jnp.float32),
        lax.psum_scatter(
            part_cross_out.astype(jnp.bfloat16), "mp", scatter_dimension=0, tiled=True
        ).astype(jnp.float32),
    )
    total_gains, total_predict, total_correct = lax.psum(
        (gain_grads, grad_predict, grad_correct), ("dp", "mp")
    )
    return (
        new_state,
        grad_state,
        grad_encoder,
        final_self_qkv,
        final_self_out,
        final_cross_qkv,
        final_cross_out,
        part_ffn_in,
        part_ffn_out,
        total_gains,
        total_predict,
        total_correct,
    )


def dot_tn(left, right):
    return lax.dot_general(
        left, right, (((0,), (0,)), ((), ())), preferred_element_type=jnp.float32
    )


def dot_nn(left, right):
    return lax.dot_general(
        left, right, (((1,), (0,)), ((), ())), preferred_element_type=jnp.float32
    )


def dot_nt(left, right):
    return lax.dot_general(
        left, right, (((1,), (1,)), ((), ())), preferred_element_type=jnp.float32
    )


def block_scores(keys_t, query, seg_ref, code_ref, block, size, high):
    scores = dot_nn(keys_t[:high], query)
    if seg_ref is None:
        return scores
    seg_query = seg_ref[:, block * size : (block + 1) * size]
    codes = jnp.concatenate([code_ref[:high, :]] * (size // 128), axis=1)
    same = codes == seg_query
    low = block * size
    key = lax.broadcasted_iota(jnp.int32, (size, size), 0)
    query_pos = lax.broadcasted_iota(jnp.int32, (size, size), 1)
    near = (same[low:] & (key <= query_pos)) | (key == query_pos)
    lower = jnp.where(near, scores[low:], MASKED_SCORE)
    if low == 0:
        return lower
    return jnp.concatenate([jnp.where(same[:low], scores[:low], MASKED_SCORE), lower], axis=0)


def attend_kernel(masked, size, *refs):
    if masked:
        q_ref, k_ref, v_ref, seg_ref, code_ref, mix_ref, log_ref = refs
    else:
        q_ref, k_ref, v_ref, mix_ref, log_ref = refs
        seg_ref = code_ref = None
    key_len, query_len = k_ref.shape[1], q_ref.shape[1]
    keys_t = k_ref[...].T
    values = v_ref[...]
    for block in range(query_len // size):
        cols = slice(block * size, (block + 1) * size)
        high = (block + 1) * size if masked else key_len
        query = q_ref[:, cols] * jnp.bfloat16(HEAD ** (-0.5))
        scores = block_scores(keys_t, query, seg_ref, code_ref, block, size, high)
        top = jnp.max(scores, axis=0, keepdims=True)
        exponent = jnp.exp(scores - top)
        total = jnp.sum(exponent, axis=0, keepdims=True)
        mixed = dot_nn(values[:, :high], exponent.astype(jnp.bfloat16))
        mix_ref[:, cols] = (mixed / total).astype(jnp.bfloat16)
        log_ref[0, :, cols] = top + jnp.log(total)


def attend_back_kernel(masked, size, *refs):
    if masked:
        q_ref, k_ref, v_ref, seg_ref, code_ref = refs[:5]
        refs = refs[5:]
    else:
        q_ref, k_ref, v_ref = refs[:3]
        seg_ref = code_ref = None
        refs = refs[3:]
    log_ref, mix_ref, grad_ref, dq_ref, dk_ref, dv_ref, dk_sum, dv_sum = refs
    key_len, query_len = k_ref.shape[1], q_ref.shape[1]
    keys = k_ref[...]
    keys_t = keys.T
    values_t = v_ref[...].T
    last = query_len // size - 1
    for block in range(last, -1, -1):
        cols = slice(block * size, (block + 1) * size)
        high = (block + 1) * size if masked else key_len
        query = q_ref[:, cols] * jnp.bfloat16(HEAD ** (-0.5))
        grad = grad_ref[:, cols]
        scores = block_scores(keys_t, query, seg_ref, code_ref, block, size, high)
        probs = jnp.exp(scores - log_ref[0, :, cols])
        grad_probs = dot_nn(values_t[:high], grad)
        row_dot = jnp.sum(
            grad.astype(jnp.float32) * mix_ref[:, cols].astype(jnp.float32), axis=0, keepdims=True
        )
        grad_scores = (probs * (grad_probs - row_dot)).astype(jnp.bfloat16)
        dq_ref[:, cols] = (dot_nn(keys[:, :high], grad_scores) * HEAD ** (-0.5)).astype(
            jnp.bfloat16
        )
        dk = dot_nt(query, grad_scores)
        dv = dot_nt(grad, probs.astype(jnp.bfloat16))
        if block == last:
            dk_sum[:, :high] = dk
            dv_sum[:, :high] = dv
        else:
            dk_sum[:, :high] += dk
            dv_sum[:, :high] += dv
    dk_ref[...] = dk_sum[...].astype(jnp.bfloat16)
    dv_ref[...] = dv_sum[...].astype(jnp.bfloat16)


def head_rows(first, length):
    return pl.BlockSpec((HEAD, length), lambda head: (first + head, 0))


def attention_call(queries, keys, values, heads, mask, back, size):
    (q_arr, q_at), (k_arr, k_at), (v_arr, v_at) = queries, keys, values
    q_len, k_len = q_arr.shape[1], k_arr.shape[1]
    operands = [q_arr, k_arr, v_arr]
    specs = [head_rows(q_at, q_len), head_rows(k_at, k_len), head_rows(v_at, k_len)]
    if mask is not None:
        operands += list(mask)
        specs += [
            pl.BlockSpec((1, q_len), lambda head: (0, 0)),
            pl.BlockSpec((k_len, 128), lambda head: (0, 0)),
        ]
    log_spec = pl.BlockSpec((1, 1, q_len), lambda head: (head, 0, 0))
    q_out = jax.ShapeDtypeStruct((heads * HEAD, q_len), jnp.bfloat16)
    k_out = jax.ShapeDtypeStruct((heads * HEAD, k_len), jnp.bfloat16)
    pairs = heads * q_len * k_len * (0.6 if mask is not None else 1.0)
    if back is None:
        kernel, dots, scratch = attend_kernel, 2, []
        out_shape = [q_out, jax.ShapeDtypeStruct((heads, 1, q_len), jnp.float32)]
        out_specs = [head_rows(0, q_len), log_spec]
    else:
        kernel, dots = attend_back_kernel, 5
        operands += list(back)
        specs += [log_spec, head_rows(0, q_len), head_rows(0, q_len)]
        out_shape = [q_out, k_out, k_out]
        out_specs = [head_rows(0, q_len), head_rows(0, k_len), head_rows(0, k_len)]
        scratch = [pltpu.VMEM((HEAD, k_len), jnp.float32)] * 2
    return pl.pallas_call(
        functools.partial(kernel, mask is not None, size),
        grid=(heads,),
        in_specs=specs,
        out_specs=out_specs,
        out_shape=out_shape,
        scratch_shapes=scratch,
        compiler_params=pltpu.CompilerParams(vmem_limit_bytes=32 << 20),
        cost_estimate=pl.CostEstimate(
            flops=int(8 * HEAD * dots * pairs),
            bytes_accessed=4 * heads * HEAD * (q_len + k_len) * dots // 2,
            transcendentals=int(pairs),
        ),
        name="attend" if back is None else "attend_back",
    )(*operands)


MESH = pl.DeviceIdType.MESH


def after(value, *earlier):
    return lax.optimization_barrier((value, *earlier))[0]


def rms_scale(values):
    return lax.rsqrt(jnp.mean(values * values, axis=0, keepdims=True) + EPSILON)


def pick(array, index, axis=0):
    return lax.dynamic_index_in_dim(array, index, axis, keepdims=False)


def all_sum_kernel(dp_size, mp_size, part_ref, out_ref, mp_slots, row_sum, dp_slots, *sems):
    mp_send, mp_recv, dp_send, dp_recv = sems
    dp, mp = lax.axis_index("dp"), lax.axis_index("mp")
    mp_peers = [lax.rem(mp + s, mp_size) for s in range(1, mp_size)]
    dp_peers = [lax.rem(dp + s, dp_size) for s in range(1, dp_size)]
    barrier = pltpu.get_barrier_semaphore()
    for peer in mp_peers:
        pl.semaphore_signal(barrier, inc=1, device_id=(dp, peer), device_id_type=MESH)
    for peer in dp_peers:
        pl.semaphore_signal(barrier, inc=1, device_id=(peer, mp), device_id_type=MESH)
    pl.semaphore_wait(barrier, mp_size + dp_size - 2)

    def exchange(source, slots, send, recv, targets):
        copies = []
        for step, target in enumerate(targets):
            copies.append(
                pltpu.make_async_remote_copy(
                    src_ref=source,
                    dst_ref=slots.at[step],
                    send_sem=send.at[step],
                    recv_sem=recv.at[step],
                    device_id=target,
                    device_id_type=MESH,
                )
            )
            copies[-1].start()
        for copy in copies:
            copy.wait()

    exchange(part_ref, mp_slots, mp_send, mp_recv, [(dp, p) for p in mp_peers])
    row_sum[...] = ordered_sum(part_ref, mp_slots, mp, mp_size)
    exchange(row_sum, dp_slots, dp_send, dp_recv, [(p, mp) for p in dp_peers])
    out_ref[...] = ordered_sum(row_sum, dp_slots, dp, dp_size)


def ordered_sum(own_ref, slots, place, size):
    total = jnp.zeros_like(own_ref)
    for device in range(size):
        term = own_ref[...]
        for step in range(size - 1):
            from_here = lax.rem(place + size - step - 1, size) == device
            term = jnp.where(from_here, slots[step], term)
        total += term
    return total


def all_sum(part, dp_size, mp_size):
    return pl.pallas_call(
        functools.partial(all_sum_kernel, dp_size, mp_size),
        out_shape=jax.ShapeDtypeStruct(part.shape, part.dtype),
        in_specs=[pl.BlockSpec(memory_space=pltpu.VMEM)],
        out_specs=pl.BlockSpec(memory_space=pltpu.VMEM),
        scratch_shapes=[
            pltpu.VMEM((mp_size - 1, *part.shape), part.dtype),
            pltpu.VMEM(part.shape, part.dtype),
            pltpu.VMEM((dp_size - 1, *part.shape), part.dtype),
            pltpu.SemaphoreType.DMA((mp_size - 1,)),
            pltpu.SemaphoreType.DMA((mp_size - 1,)),
            pltpu.SemaphoreType.DMA((dp_size - 1,)),
            pltpu.SemaphoreType.DMA((dp_size - 1,)),
        ],
        compiler_params=pltpu.CompilerParams(collective_id=0, has_side_effects=True),
        name="all_sum",
    )(part)


def row_scatter_kernel(dp_size, keep_ref, send_ref, side_ref, out_ref, side_out_ref, *scratch):
    landed, mine, step_send, step_land, far_send, far_land = scratch[:6]
    cross_sems, step_sems, far_sems = scratch[6:8], scratch[8:10], scratch[10:12]
    bf16, f32 = jnp.bfloat16, jnp.float32
    dp, mp = lax.axis_index("dp"), lax.axis_index("mp")
    chip, core = mp // 2, lax.rem(mp, 2)
    outer, inner = dp // 2, lax.rem(dp, 2)
    count = dp_size // 2
    peer = ((dp, (1 - chip) * 2 + core))
    mate = (outer * 2 + 1 - inner, mp)
    offsets = [(count // 2 + i) % count for i in range(count)]
    offsets = [o for o in offsets if o] + [0]
    places = [lax.rem(outer + o, count) for o in offsets]
    targets = [(place * 2 + inner, mp) for place in places]
    last = count - 1

    barrier = pltpu.get_barrier_semaphore()
    for device in [peer, mate] + targets[:last]:
        pl.semaphore_signal(barrier, inc=1, device_id=device, device_id_type=MESH)
    pl.semaphore_wait(barrier, count + 1)

    def remote(source, target, sems, index, device):
        return pltpu.make_async_remote_copy(
            src_ref=source,
            dst_ref=target,
            send_sem=sems[0].at[index],
            recv_sem=sems[1].at[index],
            device_id=device,
            device_id_type=MESH,
        )

    def half_block(dp_index):
        return lax.rem(dp_index // count + core, 2), lax.rem(dp_index, count)

    crossing = []
    for k, place in enumerate(places):
        for own in range(2):
            part, block = half_block(place * 2 + (inner if own else 1 - inner))
            copy = remote(
                send_ref.at[part, :, block], landed.at[2 * k + own], cross_sems, 2 * k + own, peer
            )
            copy.start()
            crossing.append(copy)
    stepping = {}
    for k, place in enumerate(places):
        stepping[0, k] = remote(
            side_ref.at[:, place * 2 + 1 - inner], step_land.at[0, k], step_sems, k, mate
        )
        stepping[0, k].start()
    going = []

    def pass_on(group, k, value, final_ref):
        stepping[group, k].wait()
        total = value.astype(f32) + step_land[group, k].astype(f32)
        if k == last:
            final_ref[...] = total
            return
        far_send[group, k] = total.astype(bf16)
        copy = remote(
            far_send.at[group, k], far_land.at[group, k], far_sems, group * last + k, targets[k]
        )
        copy.start()
        going.append((copy, final_ref, group, k))

    for k, place in enumerate(places):
        pass_on(0, k, side_ref[:, place * 2 + inner], side_out_ref)
    for k, place in enumerate(places):
        for own in range(2):
            part, block = half_block(place * 2 + (inner if own else 1 - inner))
            crossing[2 * k + own].wait()
            total = keep_ref[part, :, block].astype(f32) + landed[2 * k + own].astype(f32)
            if own:
                mine[k] = total.astype(bf16)
            else:
                step_send[k] = total.astype(bf16)
                stepping[1, k] = remote(
                    step_send.at[k], step_land.at[1, k], step_sems, count + k, mate
                )
                stepping[1, k].start()
        if k:
            pass_on(1, k - 1, mine[k - 1], out_ref)
    pass_on(1, last, mine[last], out_ref)
    for copy, final_ref, group, k in going:
        copy.wait()
        final_ref[...] += far_land[group, k].astype(f32)


def row_scatter(keep, send, side, dp_size):
    _, mats, _, rows, columns = keep.shape
    block = (mats, rows, columns)
    count = dp_size // 2
    whole = pl.BlockSpec(memory_space=pltpu.VMEM)
    shape = jax.ShapeDtypeStruct(block, jnp.float32)
    dma = pltpu.SemaphoreType.DMA
    return pl.pallas_call(
        functools.partial(row_scatter_kernel, dp_size),
        out_shape=[shape, shape],
        in_specs=[whole] * 3,
        out_specs=[whole] * 2,
        scratch_shapes=[
            pltpu.VMEM((dp_size, *block), jnp.bfloat16),
            pltpu.VMEM((count, *block), jnp.bfloat16),
            pltpu.VMEM((count, *block), jnp.bfloat16),
            pltpu.VMEM((2, count, *block), jnp.bfloat16),
            pltpu.VMEM((2, count - 1, *block), jnp.bfloat16),
            pltpu.VMEM((2, count - 1, *block), jnp.bfloat16),
            dma((dp_size,)),
            dma((dp_size,)),
            dma((2 * count,)),
            dma((2 * count,)),
            dma((2 * (count - 1),)),
            dma((2 * (count - 1),)),
        ],
        compiler_params=pltpu.CompilerParams(
            collective_id=1, has_side_effects=True, vmem_limit_bytes=40 << 20
        ),
        name="row_scatter",
    )(keep, send, side)


def join_norm_kernel(place_ref, gain_ref, *refs):
    pieces, (active_ref, normed_ref, scale_ref) = refs[:4], refs[4:]
    depth = pieces[0].shape[0]
    squares = sum(
        jnp.sum(jnp.square(p[...].astype(jnp.float32)), axis=0, keepdims=True) for p in pieces
    )
    scale = lax.rsqrt(squares * (1.0 / (4 * depth)) + EPSILON)
    scale_ref[...] = scale
    for i, piece in enumerate(pieces):
        quarter = place_ref[i]
        value = piece[...]
        active_ref[quarter] = value
        normed = value.astype(jnp.float32) * scale * gain_ref[quarter]
        normed_ref[i] = normed.astype(jnp.bfloat16)


def join_norm(places, gain, pieces):
    depth, length = pieces[0].shape
    whole = pl.BlockSpec(memory_space=pltpu.VMEM)
    full = jax.ShapeDtypeStruct((4, depth, length), jnp.bfloat16)
    return pl.pallas_call(
        join_norm_kernel,
        out_shape=[full, full, jax.ShapeDtypeStruct((1, length), jnp.float32)],
        in_specs=[pl.BlockSpec(memory_space=pltpu.SMEM)] + [whole] * 5,
        out_specs=[whole] * 3,
        cost_estimate=pl.CostEstimate(
            flops=40 * depth * length, bytes_accessed=24 * depth * length, transcendentals=length
        ),
        name="join_norm",
    )(places, gain, *pieces)


def dot_tt(left, right):
    return lax.dot_general(
        left, right, (((0,), (1,)), ((), ())), preferred_element_type=jnp.float32
    )


def outer_kernel(sizes, *refs):
    keep_ref, send_ref = refs[-2:]
    at, row = 0, 0
    for size in sizes:
        near, far = refs[at][...], refs[at + 1][...]
        for ref in refs[at + 2 : at + 2 + size]:
            for low in range(0, ref.shape[0], 384):
                block = ref[low : low + 384, :]
                rows = slice(row, row + block.shape[0])
                keep_ref[rows, :] = dot_nt(block, near).astype(jnp.bfloat16)
                send_ref[rows, :] = dot_nt(block, far).astype(jnp.bfloat16)
                row += block.shape[0]
        at += 2 + size


def outer_products(groups):
    operands, sizes, rows, flops = [], [], 0, 0
    for outer, inner in groups:
        operands += [*inner, *outer]
        sizes.append(len(outer))
        rows += sum(o.shape[0] for o in outer)
        flops += sum(4 * o.size * inner[0].shape[0] for o in outer)
    columns = operands[0].shape[0]
    whole = pl.BlockSpec(memory_space=pltpu.VMEM)
    shape = jax.ShapeDtypeStruct((rows, columns), jnp.bfloat16)
    return pl.pallas_call(
        functools.partial(outer_kernel, tuple(sizes)),
        out_shape=[shape, shape],
        in_specs=[whole] * len(operands),
        out_specs=[whole] * 2,
        compiler_params=pltpu.CompilerParams(vmem_limit_bytes=32 << 20),
        cost_estimate=pl.CostEstimate(
            flops=flops,
            bytes_accessed=sum(2 * o.size for o in operands) + 4 * rows * columns,
            transcendentals=0,
        ),
        name="outer_products",
    )(*operands)


def self_products_kernel(core_ref, *refs):
    grads, (norm_ref, near_own, near_mate, far_own, far_mate) = refs[:6], refs[6:11]
    attn_ref, mix_near, mix_far, keep_ref, send_ref, into_ref = refs[11:]
    core = core_ref[0]
    for i, ref in enumerate(grads):
        side, mat = i // 3, i % 3
        grad = ref[...]
        send_ref[side, mat] = dot_nt(grad, norm_ref[1]).astype(jnp.bfloat16)
        keep_ref[side, mat] = dot_nt(grad, norm_ref[0]).astype(jnp.bfloat16)
    for side in range(2):
        place = core if side == 0 else 1 - core
        grad = attn_ref[place]
        send_ref[side, 3] = dot_nt(grad, mix_far[...]).astype(jnp.bfloat16)
        keep_ref[side, 3] = dot_nt(grad, mix_near[...]).astype(jnp.bfloat16)
    for mat in range(3):
        joined = jnp.concatenate([grads[mat][...], grads[3 + mat][...]], axis=0)
        for out, (own, mate) in enumerate(((near_own, near_mate), (far_own, far_mate))):
            term = dot_nn(jnp.concatenate([own[mat], mate[mat]], axis=1), joined)
            if mat == 0:
                into_ref[out] = term
            else:
                into_ref[out] += term


def self_products(grads, normed, weights, grad_attn, mixes, core):
    half, length = grads[0].shape
    depth = normed.shape[1]
    whole = pl.BlockSpec(memory_space=pltpu.VMEM)
    shape = jax.ShapeDtypeStruct((2, 4, half, depth), jnp.bfloat16)
    operands = [*grads, normed, *weights, grad_attn, *mixes]
    return pl.pallas_call(
        self_products_kernel,
        out_shape=[shape, shape, jax.ShapeDtypeStruct((2, depth, length), jnp.float32)],
        in_specs=[pl.BlockSpec(memory_space=pltpu.SMEM)] + [whole] * len(operands),
        out_specs=[whole] * 3,
        compiler_params=pltpu.CompilerParams(vmem_limit_bytes=40 << 20),
        cost_estimate=pl.CostEstimate(
            flops=2 * 28 * half * length * depth,
            bytes_accessed=sum(2 * o.size for o in operands) + 8 * depth * length,
            transcendentals=0,
        ),
        name="self_products",
    )(core, *operands)


def paired_shards(
    dp_size,
    wide_state,
    encoder,
    segments,
    key_valid,
    self_qkv,
    self_out,
    cross_qkv,
    cross_out,
    ffn_in,
    ffn_out,
    norm_gains,
    predict,
    correct,
    cotangent,
):
    bf16, f32 = jnp.bfloat16, jnp.float32
    me = lax.axis_index("mp")
    chip, core = me // 2, me % 2
    far = me ^ 2
    mates = [(i, i ^ 1) for i in range(4)]
    peers = [(i, i ^ 2) for i in range(4)]

    def to_mate(array):
        return lax.ppermute(array, "mp", mates)

    def to_peer(array):
        return lax.ppermute(array, "mp", peers)

    def quarters(own, across, axis=0):
        pieces = [own, across, to_mate(own), to_mate(across)]
        stacked = jnp.stack(pieces)
        order = [pick(stacked, ((j % 2) ^ core) * 2 + ((j // 2) ^ chip)) for j in range(4)]
        return jnp.concatenate(order, axis=axis)

    def halves(own, axis=0):
        other = to_mate(own)
        return jnp.where(
            core == 0,
            jnp.concatenate([own, other], axis=axis),
            jnp.concatenate([other, own], axis=axis),
        )

    def by_row(own, other):
        return jnp.where(chip == 0, jnp.stack([own, other]), jnp.stack([other, own]))

    def project(weights, values):
        return dot_tn(weights, values)

    length = wide_state.shape[3]
    width = self_qkv.shape[2]
    depth = self_qkv.shape[1]
    half = width // 2
    heads = half // HEAD
    gains = norm_gains[:, :, None]

    block_a = wide_state[:, 0].astype(f32)
    block_b = wide_state[:, 1].astype(f32)
    guess_a = predict[0, 0] * block_a + predict[0, 1] * block_b
    guess_b = predict[1, 0] * block_a + predict[1, 1] * block_b
    active_rows = guess_a.astype(bf16)
    act_own = pick(active_rows, chip)
    act_far = to_peer(pick(active_rows, 1 - chip))
    qkv_far = to_peer(self_qkv)
    act_pieces = [act_own, act_far, to_mate(act_own), to_mate(act_far)]
    places = jnp.stack([me, far, me ^ 1, me ^ 3]).astype(jnp.int32)
    active, normed_pieces, scale_a = join_norm(
        places, norm_gains[0].reshape(4, depth, 1), act_pieces
    )
    active = active.reshape(width, length)
    normed_a = normed_pieces.reshape(width, length)
    self_out = after(self_out, qkv_far, act_far)
    self_out_far = to_peer(self_out)
    enc_far = to_peer(after(pick(encoder, 1 - chip), qkv_far, act_far))
    cross_qkv_far = to_peer(after(cross_qkv, qkv_far, act_far))
    cross_out_far = to_peer(after(cross_out, qkv_far, act_far))
    cot_a = cotangent[:, 0].astype(f32)
    cot_b = cotangent[:, 1].astype(f32)
    grad_branch = (correct[0] * cot_a + correct[1] * cot_b).astype(bf16)
    grad_far = to_peer(after(grad_branch, qkv_far, act_far))

    def columns(array, which):
        return lax.dynamic_slice_in_dim(array, which * half, half, array.ndim - 1)

    own_near, own_far = columns(self_qkv, core), columns(qkv_far, core)
    mate_near, mate_far = columns(self_qkv, 1 - core), columns(qkv_far, 1 - core)
    w_qkv = jnp.concatenate([own_near, own_far, to_mate(mate_near), to_mate(mate_far)], axis=1)
    w_self_out = quarters(self_out, self_out_far)
    enc = quarters(pick(encoder, chip), enc_far)
    w_cross = quarters(cross_qkv, cross_qkv_far, axis=1)
    w_cross_out = quarters(cross_out, cross_out_far)
    all_grad = quarters(grad_branch, grad_far, axis=1)
    grad_own = pick(all_grad, chip)
    grad_other = pick(all_grad, 1 - chip)

    resid_a = active.astype(f32)
    qkv = jnp.concatenate([project(w_qkv[i], normed_a).astype(bf16) for i in range(3)], axis=0)
    seg_row = pick(segments, chip)
    code = jnp.where(pick(key_valid, chip) > 0, seg_row, -1)
    mask = (seg_row[None], jnp.broadcast_to(code[:, None], (length, 128)))
    self_args = ((qkv, 0), (qkv, heads), (qkv, 2 * heads), heads, mask)
    mix_own, self_log = attention_call(*self_args, None, 512)
    self_mix = halves(mix_own)
    attn_out = project(w_self_out, self_mix)

    resid_b = resid_a + attn_out
    scale_b = rms_scale(resid_b)
    normed_b = (resid_b * scale_b * gains[1]).astype(bf16)
    w_cross_own = columns(w_cross, core)
    cross_q = project(w_cross_own[0], normed_b).astype(bf16)
    cross_kv = jnp.concatenate(
        [
            lax.dot_general(
                w_cross_own[i], enc, (((0,), (1,)), ((), ())), preferred_element_type=f32
            ).astype(bf16)
            for i in (1, 2)
        ],
        axis=0,
    )
    cross_args = ((cross_q, 0), (cross_kv, 0), (cross_kv, heads), heads, None)
    cmix_own, cross_log = attention_call(*cross_args, None, 512)
    cross_mix = halves(cmix_own)
    cross_res = project(w_cross_out, cross_mix)
    resid_c = resid_b + cross_res
    scale_c = rms_scale(resid_c)
    normed_own = (resid_c * scale_c * gains[2]).astype(bf16)
    branch = (attn_out + cross_res).astype(bf16)

    normed_half = lax.dynamic_slice_in_dim(normed_own, core * half, half, 0)
    normed_other = halves(to_peer(normed_half))

    def forward(normed):
        gate_pre = project(ffn_in[0], normed)
        up_pre = project(ffn_in[1], normed)
        hidden = gated_unit(gate_pre, up_pre).astype(bf16)
        return gate_pre, up_pre, hidden, project(ffn_out, hidden)

    def backward(gate_pre, up_pre, grad_rows):
        grad_hidden = dot_nn(ffn_out, grad_rows)
        _, gate_back = jax.vjp(gated_unit, gate_pre, up_pre)
        grad_gate, grad_up = (g.astype(bf16) for g in gate_back(grad_hidden))
        back = dot_nn(ffn_in[0], grad_gate) + dot_nn(ffn_in[1], grad_up)
        return grad_gate, grad_up, back

    def my_half(part):
        split = part.reshape(2, 2, depth, length)
        got = to_mate(pick(split, 1 - core, 1).astype(bf16))
        return pick(split, core, 1) + got.astype(f32)

    gate_o, up_o, hid_o, res_o = forward(normed_own)
    gg_o, gu_o, back_o = backward(gate_o, up_o, grad_own)
    normed_other = after(normed_other, gg_o, gu_o, back_o)
    gate_t, up_t, hid_t, res_t = forward(normed_other)
    gg_t, gu_t, back_t = backward(gate_t, up_t, grad_other)

    block = width // dp_size

    def joined(mats):
        return jnp.concatenate([m.reshape(dp_size, block, m.shape[1]) for m in mats], axis=1)

    def scatter(rows):
        out = lax.psum_scatter(rows, "dp", scatter_dimension=0, tiled=True)
        return out.reshape(-1, block, out.shape[2]).astype(f32)

    grad_in = [
        (dot_nt(normed_own, own) + dot_nt(normed_other, other)).astype(bf16)
        for own, other in ((gg_o, gg_t), (gu_o, gu_t))
    ]
    grad_out = (dot_nt(grad_own, hid_o) + dot_nt(grad_other, hid_t)).astype(bf16)
    ffn_joined = joined(grad_in + [grad_out])
    back_sent = my_half(back_t).astype(bf16)
    back_far = to_peer(back_sent)
    sum_o = my_half(res_o) + pick(branch.reshape(2, 2, depth, length), core, 1).astype(f32)
    sum_t = my_half(res_t)
    sum_sent = jnp.stack([pick(sum_o, 1 - chip), pick(sum_t, 1 - chip)]).astype(bf16)
    back_far, ffn_joined, sum_sent = lax.optimization_barrier(
        (back_far, ffn_joined, sum_sent)
    )
    back_half = my_half(back_o) + back_far.astype(f32)
    back_mate = to_mate(back_half.astype(bf16)).astype(f32)
    back_both = jnp.stack([back_half, back_mate])
    grad_normed_c = jnp.stack([pick(back_both, core), pick(back_both, 1 - core)], axis=1).reshape(
        width, length
    )

    ffn_parts = scatter(ffn_joined)

    sum_far = to_peer(sum_sent)
    branch_sum = by_row(
        pick(sum_o, chip) + sum_far[1].astype(f32), pick(sum_t, chip) + sum_far[0].astype(f32)
    )
    new_state = jnp.stack(
        [guess_a + correct[0] * branch_sum, guess_b + correct[1] * branch_sum], axis=1
    ).astype(bf16)
    grad_correct = jnp.stack([jnp.sum(cot_a * branch_sum), jnp.sum(cot_b * branch_sum)])


    def rms_back(values, scale, gain, incoming):
        inner = jnp.mean(gain * incoming * values, axis=0, keepdims=True)
        return (
            scale * gain * incoming - values * (scale * scale * scale) * inner,
            jnp.sum(incoming * values * scale, axis=1),
        )

    def near_far(inner):
        split = inner.reshape(4, depth, inner.shape[1])
        return pick(split, me), pick(split, far)

    grad_rows = grad_own.astype(f32)
    grad_resid_c, gain_grad_c = rms_back(resid_c, scale_c, gains[2], grad_normed_c)
    grad_cross_b = (grad_rows + grad_resid_c).astype(bf16)
    cross_out_rows = lax.dynamic_slice_in_dim(w_cross_out, core * half, half, 0)
    grad_cmix = dot_nn(cross_out_rows, grad_cross_b).astype(bf16)
    gcq, gck, gcv = attention_call(*cross_args, (cross_log, cmix_own, grad_cmix), 512)
    gcq_all, gck_all, gcv_all = halves(gcq), halves(gck), halves(gcv)
    grad_normed_b = dot_nn(w_cross[0], gcq_all)
    side_keep, side_send = outer_products(
        (
            ((gcq_all,), near_far(normed_b)),
            ((gck_all, gcv_all), near_far(enc.T)),
            ((grad_cross_b,), near_far(cross_mix)),
        )
    )
    side_sum = (side_keep.astype(f32) + to_peer(side_send).astype(f32)).astype(bf16)
    enc_rows = encoder.shape[1]

    def encoder_grad(which):
        keys = lax.dynamic_slice_in_dim(gck_all, which * enc_rows, enc_rows, 1)
        values = lax.dynamic_slice_in_dim(gcv_all, which * enc_rows, enc_rows, 1)
        return dot_tt(keys, w_cross[1]) + dot_tt(values, w_cross[2])

    enc_got = to_peer(encoder_grad(far).astype(bf16)).astype(f32)
    grad_encoder = by_row(encoder_grad(me), enc_got)

    resid_b_part, gain_grad_b = rms_back(resid_b, scale_b, gains[1], grad_normed_b)
    grad_resid_b = grad_resid_c + resid_b_part
    grad_attn_b = (grad_rows + grad_resid_b).astype(bf16)
    self_out_rows = lax.dynamic_slice_in_dim(w_self_out, core * half, half, 0)
    grad_mix = dot_nn(self_out_rows, grad_attn_b).astype(bf16)
    g_own = attention_call(*self_args, (self_log, mix_own, grad_mix), 256)
    g_mate = [to_mate(g) for g in g_own]
    keep, send, both_in = self_products(
        (*g_own, *g_mate),
        normed_pieces,
        (own_near, mate_near, own_far, mate_far),
        grad_attn_b.reshape(2, half, length),
        near_far(self_mix),
        core.astype(jnp.int32).reshape(1),
    )
    blocks = (2, 4, dp_size // 2, half // (dp_size // 2), depth)
    self_parts, side_parts = row_scatter(
        keep.reshape(blocks),
        send.reshape(blocks),
        side_sum.reshape(4, dp_size, block, depth),
        dp_size,
    )
    both_act = jnp.stack([act_own, act_far]).astype(f32)
    gain_a = norm_gains[0].reshape(4, depth)
    both_gain = jnp.stack([pick(gain_a, me), pick(gain_a, far)])[:, :, None]
    inner = jnp.sum(both_gain * both_in * both_act, axis=(0, 1))[None]
    inner = (inner + to_mate(inner)) / width
    split_b = grad_resid_b.reshape(4, depth, length)
    both_b = jnp.stack([pick(split_b, me), pick(split_b, far)])
    both_back = scale_a * both_gain * both_in - both_act * (scale_a * scale_a * scale_a) * inner
    grad_active = (both_b + both_back).astype(bf16)
    gain_sums = jnp.sum(both_in * both_act * scale_a, axis=2)
    slot = jnp.arange(4, dtype=jnp.int32)[:, None]
    gain_grad_a = (
        jnp.where(slot == me, gain_sums[0][None], 0.0)
        + jnp.where(slot == far, gain_sums[1][None], 0.0)
    ).reshape(width)

    grad_cols = by_row(grad_active[0], to_peer(grad_active[1])).astype(f32)
    grad_guess_a = cot_a + grad_cols
    grad_predict = jnp.stack(
        [
            jnp.sum(grad_guess_a * block_a),
            jnp.sum(grad_guess_a * block_b),
            jnp.sum(cot_b * block_a),
            jnp.sum(cot_b * block_b),
        ]
    )
    grad_state = jnp.stack(
        [
            predict[0, 0] * grad_guess_a + predict[1, 0] * cot_b,
            predict[0, 1] * grad_guess_a + predict[1, 1] * cot_b,
        ],
        axis=1,
    )
    scalars = jnp.concatenate([grad_predict, grad_correct, jnp.zeros((width - 6,), f32)])
    total = all_sum(
        jnp.stack([gain_grad_a, 0.5 * gain_grad_b, 0.5 * gain_grad_c, scalars]), dp_size, 4
    )

    def columns_out(part):
        return jnp.swapaxes(part, -1, -2)

    return (
        new_state,
        grad_state,
        grad_encoder,
        columns_out(self_parts[:3]),
        columns_out(self_parts[3]),
        columns_out(side_parts[:3]),
        columns_out(side_parts[3]),
        ffn_parts[:2],
        columns_out(ffn_parts[2]),
        total[:3],
        total[3, :4].reshape(2, 2),
        total[3, 4:6],
    )


def choose(paired, dp_size, wide_state, *rest):
    if paired and wide_state.shape[0] == 2:
        return paired_shards(dp_size, wide_state, *rest)
    return shards(wide_state, *rest)


def solution(mesh):
    in_specs = (
        P("dp", None, "mp", None),
        P("dp", "mp", None),
        P("dp", None),
        P("dp", None),
        P(None, "mp", None),
        P("mp", None),
        P(None, "mp", None),
        P("mp", None),
        P(None, None, "mp"),
        P("mp", None),
        P(),
        P(),
        P(),
        P("dp", None, "mp", None),
    )
    out_specs = (
        P("dp", None, "mp", None),
        P("dp", None, "mp", None),
        P("dp", "mp", None),
        P(None, "mp", "dp"),
        P("mp", "dp"),
        P(None, "mp", "dp"),
        P("mp", "dp"),
        P(None, "dp", "mp"),
        P("mp", "dp"),
        P(),
        P(),
        P(),
    )
    paired = mesh.shape["mp"] == 4
    body = functools.partial(choose, paired, mesh.shape["dp"])
    return jax.shard_map(
        body, mesh=mesh, in_specs=in_specs, out_specs=out_specs, check_vma=False
    )
```

```python
import functools

import jax
import jax.numpy as jnp
from jax import lax
from jax.experimental import pallas as pl
from jax.experimental.pallas import tpu as pltpu
from jax.sharding import PartitionSpec as P

HEADS = 12
HEAD = 64


DP, MP = "dp", "mp"
EPSILON = 1e-06
MASKED_SCORE = -1e30


def rms_norm(values, norm_gain):
    mean_sq = jnp.mean(values * values, axis=-1, keepdims=True)
    return values * lax.rsqrt(mean_sq + EPSILON) * norm_gain


def rms_back(values, norm_gain, incoming):
    _, pullback = jax.vjp(rms_norm, values, norm_gain)
    return pullback(incoming)


def gated_unit(gate_pre, up_pre):
    return jax.nn.gelu(gate_pre, approximate=True) * up_pre


def head_split(matrix):
    return matrix.reshape(matrix.shape[0], matrix.shape[1], HEADS, HEAD)


def head_join(tensor):
    return tensor.reshape(tensor.shape[0], tensor.shape[1], HEADS * HEAD)


def self_mask(segments, key_valid, query_start, query_len, key_len):
    seg_query = lax.dynamic_slice_in_dim(segments, query_start, query_len, 1)
    live_key = key_valid > 0
    query_pos = query_start + jnp.arange(query_len, dtype=jnp.int32)
    key_pos = jnp.arange(key_len, dtype=jnp.int32)
    earlier = key_pos[None, None, :] <= query_pos[None, :, None]
    itself = key_pos[None, None, :] == query_pos[None, :, None]
    same_doc = seg_query[:, :, None] == segments[:, None, :]
    return same_doc & earlier & live_key[:, None, :] | itself


def scores_of(queries, key_rows, allowed):
    scores = jnp.einsum(
        "rqhd,rkhd->rhqk",
        head_split(queries),
        head_split(key_rows),
        preferred_element_type=jnp.float32,
    ) * HEAD ** (-0.5)
    if allowed is None:
        return scores
    return jnp.where(allowed[:, None], scores, MASKED_SCORE)


def attend(queries, key_rows, value_rows, allowed):
    scores = scores_of(queries, key_rows, allowed)
    top_score = jnp.max(scores, axis=-1, keepdims=True)
    exponent = jnp.exp(scores - top_score)
    row_total = jnp.sum(exponent, axis=-1, keepdims=True)
    attn_probs = (exponent / row_total).astype(jnp.bfloat16)
    mixed_heads = jnp.einsum(
        "rhqk,rkhd->rqhd", attn_probs, head_split(value_rows), preferred_element_type=jnp.float32
    )
    return (head_join(mixed_heads).astype(jnp.bfloat16), top_score + jnp.log(row_total))


def query_side_grads(queries, key_rows, value_rows, allowed, log_total, grad_mix):
    scores = scores_of(queries, key_rows, allowed)
    attn_probs = jnp.exp(scores - log_total)
    grad_heads = head_split(grad_mix)
    grad_probs = jnp.einsum(
        "rqhd,rkhd->rhqk", grad_heads, head_split(value_rows), preferred_element_type=jnp.float32
    )
    row_dot = jnp.sum(grad_probs * attn_probs, axis=-1, keepdims=True)
    grad_scores = (attn_probs * (grad_probs - row_dot)).astype(jnp.bfloat16)
    grad_query = head_join(
        jnp.einsum(
            "rhqk,rkhd->rqhd", grad_scores, head_split(key_rows), preferred_element_type=jnp.float32
        )
    ) * HEAD ** (-0.5)
    grad_key = head_join(
        jnp.einsum(
            "rhqk,rqhd->rkhd", grad_scores, head_split(queries), preferred_element_type=jnp.float32
        )
    ) * HEAD ** (-0.5)
    grad_value = head_join(
        jnp.einsum(
            "rhqk,rqhd->rkhd",
            attn_probs.astype(jnp.bfloat16),
            grad_heads,
            preferred_element_type=jnp.float32,
        )
    )
    return (grad_query, jnp.stack([grad_key, grad_value]), row_dot)


def shards(
    wide_state,
    encoder,
    segments,
    key_valid,
    self_qkv,
    self_out,
    cross_qkv,
    cross_out,
    ffn_in,
    ffn_out,
    norm_gains,
    predict,
    correct,
    cotangent,
):
    length = segments.shape[1]
    local_len = length // lax.axis_size("mp")
    offset = lax.axis_index(MP) * local_len
    state_f = jnp.transpose(wide_state.astype(jnp.float32), (0, 3, 1, 2))
    block_a = state_f[:, :, 0]
    block_b = state_f[:, :, 1]
    guess_a = predict[0, 0] * block_a + predict[0, 1] * block_b
    guess_b = predict[1, 0] * block_a + predict[1, 1] * block_b
    w_self, w_self_out, w_cross, w_cross_out = (
        lax.all_gather(self_qkv, "mp", axis=1, tiled=True),
        lax.all_gather(self_out, "mp", axis=0, tiled=True),
        lax.all_gather(cross_qkv, "mp", axis=1, tiled=True),
        lax.all_gather(cross_out, "mp", axis=0, tiled=True),
    )
    active = lax.all_to_all(
        guess_a.astype(jnp.bfloat16), "mp", split_axis=1, concat_axis=2, tiled=True
    )
    cross_kv = jnp.einsum(
        "rsd,cde->crse", encoder, w_cross[1:], preferred_element_type=jnp.float32
    ).astype(jnp.bfloat16)
    resid_a = active.astype(jnp.float32)
    normed_a = rms_norm(resid_a, norm_gains[0]).astype(jnp.bfloat16)
    self_proj = jnp.einsum(
        "rtd,cde->crte", normed_a, w_self, preferred_element_type=jnp.float32
    ).astype(jnp.bfloat16)
    queries = self_proj[0]
    all_kv, all_ckv = (
        lax.all_gather(self_proj[1:], "mp", axis=2, tiled=True),
        lax.all_gather(cross_kv, "mp", axis=2, tiled=True),
    )
    allowed = self_mask(segments, key_valid, offset, local_len, length)
    self_mix, self_log = attend(queries, all_kv[0], all_kv[1], allowed)
    attn_out = jnp.einsum("rtd,de->rte", self_mix, w_self_out, preferred_element_type=jnp.float32)
    resid_b = resid_a + attn_out
    normed_b = rms_norm(resid_b, norm_gains[1]).astype(jnp.bfloat16)
    cross_q = jnp.einsum(
        "rtd,de->rte", normed_b, w_cross[0], preferred_element_type=jnp.float32
    ).astype(jnp.bfloat16)
    cross_mix, cross_log = attend(cross_q, all_ckv[0], all_ckv[1], None)
    cross_res = jnp.einsum(
        "rtd,de->rte", cross_mix, w_cross_out, preferred_element_type=jnp.float32
    )
    resid_c = resid_b + cross_res
    normed_c = rms_norm(resid_c, norm_gains[2]).astype(jnp.bfloat16)
    all_normed = lax.all_gather(normed_c, "mp", axis=1, tiled=True)
    gate_up = jnp.einsum("rtd,cdf->crtf", all_normed, ffn_in, preferred_element_type=jnp.float32)
    hidden = gated_unit(gate_up[0], gate_up[1]).astype(jnp.bfloat16)
    ffn_part = jnp.einsum("rtf,fd->rtd", hidden, ffn_out, preferred_element_type=jnp.float32)
    ffn_res = lax.psum_scatter(
        ffn_part.astype(jnp.bfloat16), "mp", scatter_dimension=2, tiled=True
    ).astype(jnp.float32)
    branch_rows = (attn_out + cross_res).astype(jnp.bfloat16)
    branch_cols = lax.all_to_all(branch_rows, "mp", split_axis=2, concat_axis=1, tiled=True)
    branch_sum = branch_cols.astype(jnp.float32) + ffn_res
    new_rows = jnp.stack(
        [guess_a + correct[0] * branch_sum, guess_b + correct[1] * branch_sum], axis=2
    )
    new_state = jnp.transpose(new_rows, (0, 2, 3, 1)).astype(jnp.bfloat16)
    cot_f = jnp.transpose(cotangent.astype(jnp.float32), (0, 3, 1, 2))
    cot_a = cot_f[:, :, 0]
    cot_b = cot_f[:, :, 1]
    grad_branch = (correct[0] * cot_a + correct[1] * cot_b).astype(jnp.bfloat16)
    grad_correct = jnp.stack([jnp.sum(cot_a * branch_sum), jnp.sum(cot_b * branch_sum)])
    all_grad = lax.all_gather(grad_branch, "mp", axis=2, tiled=True)
    grad_rows = lax.dynamic_slice_in_dim(all_grad, offset, local_len, 1).astype(jnp.float32)
    grad_hidden = jnp.einsum("rtd,fd->rtf", all_grad, ffn_out, preferred_element_type=jnp.float32)
    grad_ffn_out = jnp.einsum("rtf,rtd->fd", hidden, all_grad, preferred_element_type=jnp.float32)
    _, gate_back = jax.vjp(gated_unit, gate_up[0], gate_up[1])
    grad_gate, grad_up = gate_back(grad_hidden)
    grad_gate_up = jnp.stack([grad_gate, grad_up]).astype(jnp.bfloat16)
    grad_ffn_in = jnp.einsum(
        "rtd,crtf->cdf", all_normed, grad_gate_up, preferred_element_type=jnp.float32
    )
    normed_part = jnp.einsum(
        "crtf,cdf->rtd", grad_gate_up, ffn_in, preferred_element_type=jnp.float32
    )
    grad_normed_c = lax.psum_scatter(normed_part, "mp", scatter_dimension=1, tiled=True)
    grad_resid_c, gain_grad_c = rms_back(resid_c, norm_gains[2], grad_normed_c)
    grad_cross_b = (grad_rows + grad_resid_c).astype(jnp.bfloat16)
    grad_cross_out = jnp.einsum(
        "rtd,rte->de", cross_mix, grad_cross_b, preferred_element_type=jnp.float32
    )
    grad_cross_mix = jnp.einsum(
        "rte,de->rtd", grad_cross_b, w_cross_out, preferred_element_type=jnp.float32
    ).astype(jnp.bfloat16)
    grad_cq, cross_key_part, _ = query_side_grads(
        cross_q, all_ckv[0], all_ckv[1], None, cross_log, grad_cross_mix
    )
    grad_cq_b = grad_cq.astype(jnp.bfloat16)
    grad_cross_first = jnp.einsum(
        "rtd,rte->de", normed_b, grad_cq_b, preferred_element_type=jnp.float32
    )
    grad_normed_b = jnp.einsum(
        "rte,de->rtd", grad_cq_b, w_cross[0], preferred_element_type=jnp.float32
    )
    resid_b_part, gain_grad_b = rms_back(resid_b, norm_gains[1], grad_normed_b)
    grad_resid_b = grad_resid_c + resid_b_part
    grad_attn_b = (grad_rows + grad_resid_b).astype(jnp.bfloat16)
    grad_self_out = jnp.einsum(
        "rtd,rte->de", self_mix, grad_attn_b, preferred_element_type=jnp.float32
    )
    grad_self_mix = jnp.einsum(
        "rte,de->rtd", grad_attn_b, w_self_out, preferred_element_type=jnp.float32
    ).astype(jnp.bfloat16)
    grad_query, self_key_part, _ = query_side_grads(
        queries, all_kv[0], all_kv[1], allowed, self_log, grad_self_mix
    )
    own_kv, own_ckv = (
        lax.psum_scatter(
            self_key_part.astype(jnp.bfloat16), "mp", scatter_dimension=2, tiled=True
        ).astype(jnp.float32),
        lax.psum_scatter(
            cross_key_part.astype(jnp.bfloat16), "mp", scatter_dimension=2, tiled=True
        ).astype(jnp.float32),
    )
    own_kv_b = own_kv.astype(jnp.bfloat16)
    own_ckv_b = own_ckv.astype(jnp.bfloat16)
    grad_qkv_b = jnp.concatenate([grad_query.astype(jnp.bfloat16)[None], own_kv_b], axis=0)
    grad_self_qkv = jnp.einsum(
        "rtd,crte->cde", normed_a, grad_qkv_b, preferred_element_type=jnp.float32
    )
    grad_normed_a = jnp.einsum(
        "crte,cde->rtd", grad_qkv_b, w_self, preferred_element_type=jnp.float32
    )
    grad_cross_kv = jnp.einsum(
        "rsd,crse->cde", encoder, own_ckv_b, preferred_element_type=jnp.float32
    )
    grad_encoder = jnp.einsum(
        "crse,cde->rsd", own_ckv_b, w_cross[1:], preferred_element_type=jnp.float32
    )
    grad_cross_qkv = jnp.concatenate([grad_cross_first[None], grad_cross_kv], axis=0)
    resid_a_part, gain_grad_a = rms_back(resid_a, norm_gains[0], grad_normed_a)
    grad_active = (grad_resid_b + resid_a_part).astype(jnp.bfloat16)
    grad_cols = lax.all_to_all(grad_active, "mp", split_axis=2, concat_axis=1, tiled=True).astype(
        jnp.float32
    )
    grad_guess_a = cot_a + grad_cols
    grad_predict = jnp.stack(
        [
            jnp.stack([jnp.sum(grad_guess_a * block_a), jnp.sum(grad_guess_a * block_b)]),
            jnp.stack([jnp.sum(cot_b * block_a), jnp.sum(cot_b * block_b)]),
        ]
    )
    grad_rows_state = jnp.stack(
        [
            predict[0, 0] * grad_guess_a + predict[1, 0] * cot_b,
            predict[0, 1] * grad_guess_a + predict[1, 1] * cot_b,
        ],
        axis=2,
    )
    grad_state = jnp.transpose(grad_rows_state, (0, 2, 3, 1))
    gain_grads = jnp.stack([gain_grad_a, gain_grad_b, gain_grad_c])
    part_self_qkv, part_self_out, part_cross_qkv, part_cross_out, part_ffn_in, part_ffn_out = (
        lax.psum_scatter(
            grad_self_qkv.astype(jnp.bfloat16), "dp", scatter_dimension=2, tiled=True
        ).astype(jnp.float32),
        lax.psum_scatter(
            grad_self_out.astype(jnp.bfloat16), "dp", scatter_dimension=1, tiled=True
        ).astype(jnp.float32),
        lax.psum_scatter(
            grad_cross_qkv.astype(jnp.bfloat16), "dp", scatter_dimension=2, tiled=True
        ).astype(jnp.float32),
        lax.psum_scatter(
            grad_cross_out.astype(jnp.bfloat16), "dp", scatter_dimension=1, tiled=True
        ).astype(jnp.float32),
        lax.psum_scatter(
            grad_ffn_in.astype(jnp.bfloat16), "dp", scatter_dimension=1, tiled=True
        ).astype(jnp.float32),
        lax.psum_scatter(
            grad_ffn_out.astype(jnp.bfloat16), "dp", scatter_dimension=1, tiled=True
        ).astype(jnp.float32),
    )
    final_self_qkv, final_self_out, final_cross_qkv, final_cross_out = (
        lax.psum_scatter(
            part_self_qkv.astype(jnp.bfloat16), "mp", scatter_dimension=1, tiled=True
        ).astype(jnp.float32),
        lax.psum_scatter(
            part_self_out.astype(jnp.bfloat16), "mp", scatter_dimension=0, tiled=True
        ).astype(jnp.float32),
        lax.psum_scatter(
            part_cross_qkv.astype(jnp.bfloat16), "mp", scatter_dimension=1, tiled=True
        ).astype(jnp.float32),
        lax.psum_scatter(
            part_cross_out.astype(jnp.bfloat16), "mp", scatter_dimension=0, tiled=True
        ).astype(jnp.float32),
    )
    total_gains, total_predict, total_correct = lax.psum(
        (gain_grads, grad_predict, grad_correct), ("dp", "mp")
    )
    return (
        new_state,
        grad_state,
        grad_encoder,
        final_self_qkv,
        final_self_out,
        final_cross_qkv,
        final_cross_out,
        part_ffn_in,
        part_ffn_out,
        total_gains,
        total_predict,
        total_correct,
    )


def dot_tn(left, right):
    return lax.dot_general(
        left, right, (((0,), (0,)), ((), ())), preferred_element_type=jnp.float32
    )


def dot_nn(left, right):
    return lax.dot_general(
        left, right, (((1,), (0,)), ((), ())), preferred_element_type=jnp.float32
    )


def dot_nt(left, right):
    return lax.dot_general(
        left, right, (((1,), (1,)), ((), ())), preferred_element_type=jnp.float32
    )


def block_scores(keys_t, query, seg_ref, code_ref, block, size, high):
    scores = dot_nn(keys_t[:high], query)
    if seg_ref is None:
        return scores
    seg_query = seg_ref[:, block * size : (block + 1) * size]
    codes = jnp.concatenate([code_ref[:high, :]] * (size // 128), axis=1)
    same = codes == seg_query
    low = block * size
    key = lax.broadcasted_iota(jnp.int32, (size, size), 0)
    query_pos = lax.broadcasted_iota(jnp.int32, (size, size), 1)
    near = (same[low:] & (key <= query_pos)) | (key == query_pos)
    lower = jnp.where(near, scores[low:], MASKED_SCORE)
    if low == 0:
        return lower
    return jnp.concatenate([jnp.where(same[:low], scores[:low], MASKED_SCORE), lower], axis=0)


def attend_kernel(masked, size, *refs):
    if masked:
        q_ref, k_ref, v_ref, seg_ref, code_ref, mix_ref, log_ref = refs
    else:
        q_ref, k_ref, v_ref, mix_ref, log_ref = refs
        seg_ref = code_ref = None
    key_len, query_len = k_ref.shape[1], q_ref.shape[1]
    keys_t = k_ref[...].T
    values = v_ref[...]
    for block in range(query_len // size):
        cols = slice(block * size, (block + 1) * size)
        high = (block + 1) * size if masked else key_len
        query = q_ref[:, cols] * jnp.bfloat16(HEAD ** (-0.5))
        scores = block_scores(keys_t, query, seg_ref, code_ref, block, size, high)
        top = jnp.max(scores, axis=0, keepdims=True)
        exponent = jnp.exp(scores - top)
        total = jnp.sum(exponent, axis=0, keepdims=True)
        mixed = dot_nn(values[:, :high], exponent.astype(jnp.bfloat16))
        mix_ref[:, cols] = (mixed / total).astype(jnp.bfloat16)
        log_ref[0, :, cols] = top + jnp.log(total)


def attend_back_kernel(masked, size, *refs):
    if masked:
        q_ref, k_ref, v_ref, seg_ref, code_ref = refs[:5]
        refs = refs[5:]
    else:
        q_ref, k_ref, v_ref = refs[:3]
        seg_ref = code_ref = None
        refs = refs[3:]
    log_ref, mix_ref, grad_ref, dq_ref, dk_ref, dv_ref, dk_sum, dv_sum = refs
    key_len, query_len = k_ref.shape[1], q_ref.shape[1]
    keys = k_ref[...]
    keys_t = keys.T
    values_t = v_ref[...].T
    last = query_len // size - 1
    for block in range(last, -1, -1):
        cols = slice(block * size, (block + 1) * size)
        high = (block + 1) * size if masked else key_len
        query = q_ref[:, cols] * jnp.bfloat16(HEAD ** (-0.5))
        grad = grad_ref[:, cols]
        scores = block_scores(keys_t, query, seg_ref, code_ref, block, size, high)
        probs = jnp.exp(scores - log_ref[0, :, cols])
        grad_probs = dot_nn(values_t[:high], grad)
        row_dot = jnp.sum(
            grad.astype(jnp.float32) * mix_ref[:, cols].astype(jnp.float32), axis=0, keepdims=True
        )
        grad_scores = (probs * (grad_probs - row_dot)).astype(jnp.bfloat16)
        dq_ref[:, cols] = (dot_nn(keys[:, :high], grad_scores) * HEAD ** (-0.5)).astype(
            jnp.bfloat16
        )
        dk = dot_nt(query, grad_scores)
        dv = dot_nt(grad, probs.astype(jnp.bfloat16))
        if block == last:
            dk_sum[:, :high] = dk
            dv_sum[:, :high] = dv
        else:
            dk_sum[:, :high] += dk
            dv_sum[:, :high] += dv
    dk_ref[...] = dk_sum[...].astype(jnp.bfloat16)
    dv_ref[...] = dv_sum[...].astype(jnp.bfloat16)


def head_rows(first, length):
    return pl.BlockSpec((HEAD, length), lambda head: (first + head, 0))


def attention_call(queries, keys, values, heads, mask, back, size):
    (q_arr, q_at), (k_arr, k_at), (v_arr, v_at) = queries, keys, values
    q_len, k_len = q_arr.shape[1], k_arr.shape[1]
    operands = [q_arr, k_arr, v_arr]
    specs = [head_rows(q_at, q_len), head_rows(k_at, k_len), head_rows(v_at, k_len)]
    if mask is not None:
        operands += list(mask)
        specs += [
            pl.BlockSpec((1, q_len), lambda head: (0, 0)),
            pl.BlockSpec((k_len, 128), lambda head: (0, 0)),
        ]
    log_spec = pl.BlockSpec((1, 1, q_len), lambda head: (head, 0, 0))
    q_out = jax.ShapeDtypeStruct((heads * HEAD, q_len), jnp.bfloat16)
    k_out = jax.ShapeDtypeStruct((heads * HEAD, k_len), jnp.bfloat16)
    pairs = heads * q_len * k_len * (0.6 if mask is not None else 1.0)
    if back is None:
        kernel, dots, scratch = attend_kernel, 2, []
        out_shape = [q_out, jax.ShapeDtypeStruct((heads, 1, q_len), jnp.float32)]
        out_specs = [head_rows(0, q_len), log_spec]
    else:
        kernel, dots = attend_back_kernel, 5
        operands += list(back)
        specs += [log_spec, head_rows(0, q_len), head_rows(0, q_len)]
        out_shape = [q_out, k_out, k_out]
        out_specs = [head_rows(0, q_len), head_rows(0, k_len), head_rows(0, k_len)]
        scratch = [pltpu.VMEM((HEAD, k_len), jnp.float32)] * 2
    return pl.pallas_call(
        functools.partial(kernel, mask is not None, size),
        grid=(heads,),
        in_specs=specs,
        out_specs=out_specs,
        out_shape=out_shape,
        scratch_shapes=scratch,
        compiler_params=pltpu.CompilerParams(vmem_limit_bytes=32 << 20),
        cost_estimate=pl.CostEstimate(
            flops=int(8 * HEAD * dots * pairs),
            bytes_accessed=4 * heads * HEAD * (q_len + k_len) * dots // 2,
            transcendentals=int(pairs),
        ),
        name="attend" if back is None else "attend_back",
    )(*operands)


MESH = pl.DeviceIdType.MESH


def after(value, *earlier):
    return lax.optimization_barrier((value, *earlier))[0]


def rms_scale(values):
    return lax.rsqrt(jnp.mean(values * values, axis=0, keepdims=True) + EPSILON)


def pick(array, index, axis=0):
    return lax.dynamic_index_in_dim(array, index, axis, keepdims=False)


def all_sum_kernel(dp_size, mp_size, part_ref, out_ref, mp_slots, row_sum, dp_slots, *sems):
    mp_send, mp_recv, dp_send, dp_recv = sems
    dp, mp = lax.axis_index(DP), lax.axis_index(MP)
    mp_peers = [lax.rem(mp + s, mp_size) for s in range(1, mp_size)]
    dp_peers = [lax.rem(dp + s, dp_size) for s in range(1, dp_size)]
    barrier = pltpu.get_barrier_semaphore()
    for peer in mp_peers:
        pl.semaphore_signal(barrier, inc=1, device_id=(dp, peer), device_id_type=MESH)
    for peer in dp_peers:
        pl.semaphore_signal(barrier, inc=1, device_id=(peer, mp), device_id_type=MESH)
    pl.semaphore_wait(barrier, mp_size + dp_size - 2)

    def exchange(source, slots, send, recv, targets):
        copies = []
        for step, target in enumerate(targets):
            copies.append(
                pltpu.make_async_remote_copy(
                    src_ref=source,
                    dst_ref=slots.at[step],
                    send_sem=send.at[step],
                    recv_sem=recv.at[step],
                    device_id=target,
                    device_id_type=MESH,
                )
            )
            copies[-1].start()
        for copy in copies:
            copy.wait()

    exchange(part_ref, mp_slots, mp_send, mp_recv, [(dp, p) for p in mp_peers])
    row_sum[...] = ordered_sum(part_ref, mp_slots, mp, mp_size)
    exchange(row_sum, dp_slots, dp_send, dp_recv, [(p, mp) for p in dp_peers])
    out_ref[...] = ordered_sum(row_sum, dp_slots, dp, dp_size)


def ordered_sum(own_ref, slots, place, size):
    total = jnp.zeros_like(own_ref)
    for device in range(size):
        term = own_ref[...]
        for step in range(size - 1):
            from_here = lax.rem(place + size - step - 1, size) == device
            term = jnp.where(from_here, slots[step], term)
        total += term
    return total


def all_sum(part, dp_size, mp_size):
    return pl.pallas_call(
        functools.partial(all_sum_kernel, dp_size, mp_size),
        out_shape=jax.ShapeDtypeStruct(part.shape, part.dtype),
        in_specs=[pl.BlockSpec(memory_space=pltpu.VMEM)],
        out_specs=pl.BlockSpec(memory_space=pltpu.VMEM),
        scratch_shapes=[
            pltpu.VMEM((mp_size - 1, *part.shape), part.dtype),
            pltpu.VMEM(part.shape, part.dtype),
            pltpu.VMEM((dp_size - 1, *part.shape), part.dtype),
            pltpu.SemaphoreType.DMA((mp_size - 1,)),
            pltpu.SemaphoreType.DMA((mp_size - 1,)),
            pltpu.SemaphoreType.DMA((dp_size - 1,)),
            pltpu.SemaphoreType.DMA((dp_size - 1,)),
        ],
        compiler_params=pltpu.CompilerParams(collective_id=0, has_side_effects=True),
        name="all_sum",
    )(part)


def finish_kernel(dp_size, keep_ref, got_ref, *refs):
    side_refs, ffn_refs = refs[:4], refs[4:8]
    qkv_out, out_out, cross_out, cross_out_out, in_out, down_out = refs[8:14]
    step_send, step_land, far_send, far_land = refs[14:18]
    step_sems, far_sems = refs[18:20], refs[20:22]
    bf16, f32 = jnp.bfloat16, jnp.float32
    dp, mp = lax.axis_index(DP), lax.axis_index(MP)
    core = lax.rem(mp, 2)
    outer, inner = dp // 2, lax.rem(dp, 2)
    count = dp_size // 2
    mate = (outer * 2 + 1 - inner, mp)
    offsets = [(count // 2 + i) % count for i in range(count)]
    offsets = [o for o in offsets if o] + [0]
    places = [lax.rem(outer + o, count) for o in offsets]
    targets = [(place * 2 + inner, mp) for place in places]
    last = count - 1

    barrier = pltpu.get_barrier_semaphore()
    for device in [mate] + targets[:last]:
        pl.semaphore_signal(barrier, inc=1, device_id=device, device_id_type=MESH)
    pl.semaphore_wait(barrier, count)

    def remote(source, target, sems, index, device):
        return pltpu.make_async_remote_copy(
            src_ref=source,
            dst_ref=target,
            send_sem=sems[0].at[index],
            recv_sem=sems[1].at[index],
            device_id=device,
            device_id_type=MESH,
        )

    def summed(place, own):
        index = place * 2 + (inner if own else 1 - inner)
        part, block = lax.rem(index // count + core, 2), lax.rem(index, count)
        return keep_ref[part, :, block].astype(f32) + got_ref[part, :, block].astype(f32)

    stepping = []
    for k, place in enumerate(places):
        step_send[k] = summed(place, False).astype(bf16)
        stepping.append(remote(step_send.at[k], step_land.at[k], step_sems, k, mate))
        stepping[k].start()

    def turned(pairs, first, second):
        depth = first.shape[1]
        for pair in range(2):
            flipped = pairs[pair].T
            for side in range(2):
                mat = 2 * pair + side
                piece = flipped[side * depth : (side + 1) * depth]
                if mat < 3:
                    first[mat] = piece
                else:
                    second[...] = piece

    turned(sum(ref[...].astype(f32) for ref in side_refs), cross_out, cross_out_out)
    for mat in range(2):
        in_out[mat] = sum(ref[mat].astype(f32) for ref in ffn_refs)
    down_out[...] = sum(ref[2].astype(f32) for ref in ffn_refs).T

    going = []
    for k, place in enumerate(places):
        stepping[k].wait()
        total = summed(place, True) + step_land[k].astype(f32)
        if k == last:
            continue
        far_send[k] = total.astype(bf16)
        going.append(remote(far_send.at[k], far_land.at[k], far_sems, k, targets[k]))
        going[k].start()
    for k, copy in enumerate(going):
        copy.wait()
        total += far_land[k].astype(f32)
    turned(total, qkv_out, out_out)


def finish(keep, got, side_terms, ffn_terms, dp_size):
    pairs, _, rows, columns = keep.shape[1:]
    depth, width = columns // 2, ffn_terms[0].shape[2]
    block = (pairs, rows, columns)
    count = dp_size // 2
    whole = pl.BlockSpec(memory_space=pltpu.VMEM)
    dma = pltpu.SemaphoreType.DMA
    three, one = (3, depth, rows), (depth, rows)
    shapes = [three, one, three, one, (2, rows, width), (width, rows)]
    return pl.pallas_call(
        functools.partial(finish_kernel, dp_size),
        out_shape=[jax.ShapeDtypeStruct(shape, jnp.float32) for shape in shapes],
        in_specs=[whole] * 10,
        out_specs=[whole] * 6,
        scratch_shapes=[
            pltpu.VMEM((count, *block), jnp.bfloat16),
            pltpu.VMEM((count, *block), jnp.bfloat16),
            pltpu.VMEM((count - 1, *block), jnp.bfloat16),
            pltpu.VMEM((count - 1, *block), jnp.bfloat16),
            dma((count,)),
            dma((count,)),
            dma((count - 1,)),
            dma((count - 1,)),
        ],
        compiler_params=pltpu.CompilerParams(
            collective_id=1, has_side_effects=True, vmem_limit_bytes=40 << 20
        ),
        name="finish",
    )(keep, got, *side_terms, *ffn_terms)


def join_norm_kernel(place_ref, gain_ref, *refs):
    pieces, (active_ref, normed_ref, scale_ref) = refs[:4], refs[4:]
    depth = pieces[0].shape[0]
    squares = sum(
        jnp.sum(jnp.square(p[...].astype(jnp.float32)), axis=0, keepdims=True) for p in pieces
    )
    scale = lax.rsqrt(squares * (1.0 / (4 * depth)) + EPSILON)
    scale_ref[...] = scale
    for i, piece in enumerate(pieces):
        quarter = place_ref[i]
        value = piece[...]
        active_ref[quarter] = value
        normed = value.astype(jnp.float32) * scale * gain_ref[quarter]
        normed_ref[i] = normed.astype(jnp.bfloat16)


def join_norm(places, gain, pieces):
    depth, length = pieces[0].shape
    whole = pl.BlockSpec(memory_space=pltpu.VMEM)
    full = jax.ShapeDtypeStruct((4, depth, length), jnp.bfloat16)
    return pl.pallas_call(
        join_norm_kernel,
        out_shape=[full, full, jax.ShapeDtypeStruct((1, length), jnp.float32)],
        in_specs=[pl.BlockSpec(memory_space=pltpu.SMEM)] + [whole] * 5,
        out_specs=[whole] * 3,
        cost_estimate=pl.CostEstimate(
            flops=40 * depth * length, bytes_accessed=24 * depth * length, transcendentals=length
        ),
        name="join_norm",
    )(places, gain, *pieces)


def dot_tt(left, right):
    return lax.dot_general(
        left, right, (((0,), (1,)), ((), ())), preferred_element_type=jnp.float32
    )


def outer_kernel(sizes, *refs):
    keep_ref, send_ref = refs[-2:]
    depth = refs[0].shape[0]
    at, mat = 0, 0
    for size in sizes:
        near, far = refs[at][...], refs[at + 1][...]
        for ref in refs[at + 2 : at + 2 + size]:
            columns = slice(mat % 2 * depth, (mat % 2 + 1) * depth)
            for low in range(0, ref.shape[0], 384):
                block = ref[low : low + 384, :]
                rows = slice(low, low + block.shape[0])
                keep_ref[mat // 2, rows, columns] = dot_nt(block, near).astype(jnp.bfloat16)
                send_ref[mat // 2, rows, columns] = dot_nt(block, far).astype(jnp.bfloat16)
            mat += 1
        at += 2 + size


def outer_products(groups):
    operands, sizes, flops = [], [], 0
    for outer, inner in groups:
        operands += [*inner, *outer]
        sizes.append(len(outer))
        flops += sum(4 * o.size * inner[0].shape[0] for o in outer)
    rows, columns = groups[0][0][0].shape[0], 2 * operands[0].shape[0]
    whole = pl.BlockSpec(memory_space=pltpu.VMEM)
    shape = jax.ShapeDtypeStruct((sum(sizes) // 2, rows, columns), jnp.bfloat16)
    return pl.pallas_call(
        functools.partial(outer_kernel, tuple(sizes)),
        out_shape=[shape, shape],
        in_specs=[whole] * len(operands),
        out_specs=[whole] * 2,
        compiler_params=pltpu.CompilerParams(vmem_limit_bytes=32 << 20),
        cost_estimate=pl.CostEstimate(
            flops=flops,
            bytes_accessed=sum(2 * o.size for o in operands) + 4 * shape.size,
            transcendentals=0,
        ),
        name="outer_products",
    )(*operands)


def self_products_kernel(core_ref, *refs):
    grads, (norm_ref, attn_ref, mix_ref, out_ref) = refs[:6], refs[6:]
    core = core_ref[0]
    depth = norm_ref.shape[0]
    norm, mix = norm_ref[...], mix_ref[...]
    for side in range(2):
        grad_rows = [ref[...] for ref in grads[3 * side : 3 * side + 3]]
        grad_rows.append(attn_ref[core if side == 0 else 1 - core])
        for mat, grad in enumerate(grad_rows):
            columns = slice(mat % 2 * depth, (mat % 2 + 1) * depth)
            value = dot_nt(grad, mix if mat == 3 else norm)
            out_ref[side, mat // 2, :, columns] = value.astype(jnp.bfloat16)


def self_products(grads, normed, grad_attn, mix, core):
    half, length = grads[0].shape
    depth = normed.shape[0]
    whole = pl.BlockSpec(memory_space=pltpu.VMEM)
    operands = [*grads, normed, grad_attn, mix]
    shape = jax.ShapeDtypeStruct((2, 2, half, 2 * depth), jnp.bfloat16)
    return pl.pallas_call(
        self_products_kernel,
        out_shape=shape,
        in_specs=[pl.BlockSpec(memory_space=pltpu.SMEM)] + [whole] * len(operands),
        out_specs=whole,
        compiler_params=pltpu.CompilerParams(vmem_limit_bytes=32 << 20),
        cost_estimate=pl.CostEstimate(
            flops=16 * half * length * depth,
            bytes_accessed=sum(2 * o.size for o in operands) + 2 * shape.size,
            transcendentals=0,
        ),
        name="self_products",
    )(core, *operands)


def into_kernel(*refs):
    grads, (near_own, near_mate, far_own, far_mate, into_ref) = refs[:6], refs[6:]
    for mat in range(3):
        joined = jnp.concatenate([grads[mat][...], grads[3 + mat][...]], axis=0)
        for out, (own, mate) in enumerate(((near_own, near_mate), (far_own, far_mate))):
            term = dot_nn(jnp.concatenate([own[mat], mate[mat]], axis=1), joined)
            if mat == 0:
                into_ref[out] = term
            else:
                into_ref[out] += term


def into_active(grads, weights):
    half, length = grads[0].shape
    depth = weights[0].shape[1]
    whole = pl.BlockSpec(memory_space=pltpu.VMEM)
    operands = [*grads, *weights]
    return pl.pallas_call(
        into_kernel,
        out_shape=jax.ShapeDtypeStruct((2, depth, length), jnp.float32),
        in_specs=[whole] * len(operands),
        out_specs=whole,
        compiler_params=pltpu.CompilerParams(vmem_limit_bytes=32 << 20),
        cost_estimate=pl.CostEstimate(
            flops=24 * half * length * depth,
            bytes_accessed=sum(2 * o.size for o in operands) + 8 * depth * length,
            transcendentals=0,
        ),
        name="into_active",
    )(*operands)


def state_grads_kernel(predict_ref, chip_ref, state_ref, cot_ref, own_ref, far_ref, out_ref, sum_ref):
    row = pl.program_id(0)
    own_row = row == chip_ref[0]
    grad = jnp.where(own_row, own_ref[...], far_ref[...]).astype(jnp.float32)
    for j in range(2):
        sum_ref[row, j] = jnp.sum(grad * state_ref[0, j].astype(jnp.float32))
    guess_a = cot_ref[0, 0].astype(jnp.float32) + grad
    guess_b = cot_ref[0, 1].astype(jnp.float32)
    for j in range(2):
        out_ref[0, j] = predict_ref[0, j] * guess_a + predict_ref[1, j] * guess_b


def state_grads(predict, chip, wide_state, cotangent, own, far):
    rows, blocks, depth, length = wide_state.shape
    smem = pl.BlockSpec(memory_space=pltpu.SMEM)
    one_row = pl.BlockSpec((1, blocks, depth, length), lambda row: (row, 0, 0, 0))
    whole = pl.BlockSpec((depth, length), lambda row: (0, 0))
    return pl.pallas_call(
        state_grads_kernel,
        grid=(rows,),
        out_shape=[
            jax.ShapeDtypeStruct(wide_state.shape, jnp.float32),
            jax.ShapeDtypeStruct((rows, blocks), jnp.float32),
        ],
        in_specs=[smem, smem, one_row, one_row, whole, whole],
        out_specs=[one_row, smem],
        compiler_params=pltpu.CompilerParams(vmem_limit_bytes=32 << 20),
        cost_estimate=pl.CostEstimate(
            flops=12 * wide_state.size, bytes_accessed=9 * wide_state.size, transcendentals=0
        ),
        name="state_grads",
    )(predict, chip, wide_state, cotangent, own, far)


def paired_shards(
    dp_size,
    wide_state,
    encoder,
    segments,
    key_valid,
    self_qkv,
    self_out,
    cross_qkv,
    cross_out,
    ffn_in,
    ffn_out,
    norm_gains,
    predict,
    correct,
    cotangent,
):
    bf16, f32 = jnp.bfloat16, jnp.float32
    me = lax.axis_index(MP)
    chip, core = me // 2, me % 2
    far = me ^ 2
    mates = [(i, i ^ 1) for i in range(4)]
    peers = [(i, i ^ 2) for i in range(4)]

    def to_mate(array):
        return lax.ppermute(array, MP, mates)

    def to_peer(array):
        return lax.ppermute(array, MP, peers)

    def quarters(own, across, axis=0):
        pieces = [own, across, to_mate(own), to_mate(across)]
        stacked = jnp.stack(pieces)
        order = [pick(stacked, ((j % 2) ^ core) * 2 + ((j // 2) ^ chip)) for j in range(4)]
        return jnp.concatenate(order, axis=axis)

    def halves(own, axis=0):
        other = to_mate(own)
        return jnp.where(
            core == 0,
            jnp.concatenate([own, other], axis=axis),
            jnp.concatenate([other, own], axis=axis),
        )

    def by_row(own, other):
        return jnp.where(chip == 0, jnp.stack([own, other]), jnp.stack([other, own]))

    def project(weights, values):
        return dot_tn(weights, values)

    length = wide_state.shape[3]
    width = self_qkv.shape[2]
    depth = self_qkv.shape[1]
    half = width // 2
    heads = half // HEAD
    gains = norm_gains[:, :, None]

    block_a = wide_state[:, 0].astype(f32)
    block_b = wide_state[:, 1].astype(f32)
    guess_a = predict[0, 0] * block_a + predict[0, 1] * block_b
    guess_b = predict[1, 0] * block_a + predict[1, 1] * block_b
    active_rows = guess_a.astype(bf16)
    act_own = pick(active_rows, chip)
    act_far = to_peer(pick(active_rows, 1 - chip))
    qkv_far = to_peer(self_qkv)
    cot_a = cotangent[:, 0].astype(f32)
    cot_b = cotangent[:, 1].astype(f32)
    grad_branch = (correct[0] * cot_a + correct[1] * cot_b).astype(bf16)
    early_sums = [jnp.sum(c * b) for c in (cot_a, cot_b) for b in (block_a, block_b)]
    seg_row = pick(segments, chip)
    code = jnp.where(pick(key_valid, chip) > 0, seg_row, -1)
    mask = (seg_row[None], jnp.broadcast_to(code[:, None], (wide_state.shape[3], 128)))
    act_far, grad_branch, early_sums, mask = lax.optimization_barrier(
        (act_far, grad_branch, early_sums, mask)
    )
    act_pieces = [act_own, act_far, to_mate(act_own), to_mate(act_far)]
    places = jnp.stack([me, far, me ^ 1, me ^ 3]).astype(jnp.int32)
    active, normed_pieces, scale_a = join_norm(
        places, norm_gains[0].reshape(4, depth, 1), act_pieces
    )
    active = active.reshape(width, length)
    normed_a = normed_pieces.reshape(width, length)
    self_out_far = to_peer(self_out)
    enc_far = to_peer(pick(encoder, 1 - chip))
    cross_qkv_far = to_peer(cross_qkv)
    cross_out_far = to_peer(cross_out)
    grad_far = to_peer(grad_branch)

    def columns(array, which):
        return lax.dynamic_slice_in_dim(array, which * half, half, array.ndim - 1)

    own_near, own_far = columns(self_qkv, core), columns(qkv_far, core)
    mate_near, mate_far = columns(self_qkv, 1 - core), columns(qkv_far, 1 - core)
    w_qkv = jnp.concatenate([own_near, own_far, to_mate(mate_near), to_mate(mate_far)], axis=1)
    w_self_out = quarters(self_out, self_out_far)
    enc = quarters(pick(encoder, chip), enc_far)
    w_cross = quarters(cross_qkv, cross_qkv_far, axis=1)
    w_cross_out = quarters(cross_out, cross_out_far)
    all_grad = quarters(grad_branch, grad_far, axis=1)
    grad_own = pick(all_grad, chip)
    grad_other = pick(all_grad, 1 - chip)

    resid_a = active.astype(f32)
    qkv = jnp.concatenate([project(w_qkv[i], normed_a).astype(bf16) for i in range(3)], axis=0)
    self_args = ((qkv, 0), (qkv, heads), (qkv, 2 * heads), heads, mask)
    mix_own, self_log = attention_call(*self_args, None, 512)
    self_mix = halves(mix_own)
    attn_out = project(w_self_out, self_mix)

    resid_b = resid_a + attn_out
    scale_b = rms_scale(resid_b)
    normed_b = (resid_b * scale_b * gains[1]).astype(bf16)
    w_cross_own = columns(w_cross, core)
    cross_q = project(w_cross_own[0], normed_b).astype(bf16)
    cross_kv = jnp.concatenate(
        [
            lax.dot_general(
                w_cross_own[i], enc, (((0,), (1,)), ((), ())), preferred_element_type=f32
            ).astype(bf16)
            for i in (1, 2)
        ],
        axis=0,
    )
    cross_args = ((cross_q, 0), (cross_kv, 0), (cross_kv, heads), heads, None)
    cmix_own, cross_log = attention_call(*cross_args, None, 512)
    cross_mix = halves(cmix_own)
    cross_res = project(w_cross_out, cross_mix)
    resid_c = resid_b + cross_res
    scale_c = rms_scale(resid_c)
    normed_own = (resid_c * scale_c * gains[2]).astype(bf16)
    branch = (attn_out + cross_res).astype(bf16)

    normed_half = lax.dynamic_slice_in_dim(normed_own, core * half, half, 0)
    normed_other = halves(to_peer(normed_half))

    def forward(normed):
        gate_pre = project(ffn_in[0], normed)
        up_pre = project(ffn_in[1], normed)
        hidden = gated_unit(gate_pre, up_pre).astype(bf16)
        return gate_pre, up_pre, hidden, project(ffn_out, hidden)

    def backward(gate_pre, up_pre, grad_rows):
        grad_hidden = dot_nn(ffn_out, grad_rows)
        _, gate_back = jax.vjp(gated_unit, gate_pre, up_pre)
        grad_gate, grad_up = (g.astype(bf16) for g in gate_back(grad_hidden))
        back = dot_nn(ffn_in[0], grad_gate) + dot_nn(ffn_in[1], grad_up)
        return grad_gate, grad_up, back

    def my_half(part):
        split = part.reshape(2, 2, depth, length)
        got = to_mate(pick(split, 1 - core, 1).astype(bf16))
        return pick(split, core, 1) + got.astype(f32)

    block = width // dp_size

    place = lax.axis_index(DP)
    outer, inner = place // 2, place % 2
    count = dp_size // 2

    def dp_start(mats):
        split = mats.reshape(mats.shape[0], count, 2, *mats.shape[2:])
        swap = [(i, i ^ 1) for i in range(dp_size)]
        sent = pick(split, 1 - inner, 2)
        got = lax.ppermute(sent, DP, swap)
        return pick(split, inner, 2), sent, got

    def dp_terms(started):
        mine = (started[0].astype(f32) + started[2].astype(f32)).astype(bf16)
        terms = [pick(mine, outer, 1)]
        for o in [(count // 2 + i) % count for i in range(count)]:
            if o:
                turn = [(i, (i + 2 * o) % dp_size) for i in range(dp_size)]
                terms.append(lax.ppermute(pick(mine, (outer + o) % count, 1), DP, turn))
        return terms

    def near_far(inner):
        split = inner.reshape(4, depth, inner.shape[1])
        return pick(split, me), pick(split, far)

    gate_o, up_o, hid_o, res_o = forward(normed_own)
    gg_o, gu_o, back_o = backward(gate_o, up_o, grad_own)
    normed_other = after(normed_other, gg_o, gu_o, back_o)
    gate_t, up_t, hid_t, res_t = forward(normed_other)
    gg_t, gu_t, back_t = backward(gate_t, up_t, grad_other)

    grad_in = [
        (dot_nt(normed_own, own) + dot_nt(normed_other, other)).astype(bf16)
        for own, other in ((gg_o, gg_t), (gu_o, gu_t))
    ]
    grad_out = (dot_nt(grad_own, hid_o) + dot_nt(grad_other, hid_t)).astype(bf16)
    ffn_joined = jnp.stack(grad_in + [grad_out]).reshape(3, dp_size, block, width)
    back_sent = my_half(back_t).astype(bf16)
    back_far = to_peer(back_sent)
    sum_o = my_half(res_o) + pick(branch.reshape(2, 2, depth, length), core, 1).astype(f32)
    sum_t = my_half(res_t)
    sum_sent = jnp.stack([pick(sum_o, 1 - chip), pick(sum_t, 1 - chip)]).astype(bf16)
    ffn_started = dp_start(ffn_joined)
    enc_near_far = near_far(enc.T)
    back_far, sum_sent, enc_near_far, _ = lax.optimization_barrier(
        (back_far, sum_sent, enc_near_far, ffn_started[1])
    )
    back_half = my_half(back_o) + back_far.astype(f32)
    back_mate = to_mate(back_half.astype(bf16)).astype(f32)
    back_both = jnp.stack([back_half, back_mate])
    grad_normed_c = jnp.stack([pick(back_both, core), pick(back_both, 1 - core)], axis=1).reshape(
        width, length
    )

    ffn_terms = dp_terms(ffn_started)

    sum_far = to_peer(sum_sent)


    def rms_back(values, scale, gain, incoming):
        inner = jnp.mean(gain * incoming * values, axis=0, keepdims=True)
        return (
            scale * gain * incoming - values * (scale * scale * scale) * inner,
            jnp.sum(incoming * values * scale, axis=1),
        )

    grad_rows = grad_own.astype(f32)
    grad_resid_c, gain_grad_c = rms_back(resid_c, scale_c, gains[2], grad_normed_c)
    grad_cross_b = (grad_rows + grad_resid_c).astype(bf16)
    cross_out_rows = lax.dynamic_slice_in_dim(w_cross_out, core * half, half, 0)
    grad_cmix = dot_nn(cross_out_rows, grad_cross_b).astype(bf16)
    gcq, gck, gcv = attention_call(*cross_args, (cross_log, cmix_own, grad_cmix), 512)
    gcq_all, gck_all, gcv_all = halves(gcq), halves(gck), halves(gcv)
    grad_normed_b = dot_nn(w_cross[0], gcq_all)
    side_keep, side_send = outer_products(
        (
            ((gcq_all,), near_far(normed_b)),
            ((gck_all, gcv_all), enc_near_far),
            ((grad_cross_b,), near_far(cross_mix)),
        )
    )
    side_got = to_peer(side_send)
    enc_rows = encoder.shape[1]

    def encoder_grad(which):
        keys = lax.dynamic_slice_in_dim(gck_all, which * enc_rows, enc_rows, 1)
        values = lax.dynamic_slice_in_dim(gcv_all, which * enc_rows, enc_rows, 1)
        return dot_tt(keys, w_cross[1]) + dot_tt(values, w_cross[2])

    enc_got = to_peer(encoder_grad(far).astype(bf16))

    resid_b_part, gain_grad_b = rms_back(resid_b, scale_b, gains[1], grad_normed_b)
    grad_resid_b = grad_resid_c + resid_b_part
    grad_attn_b = (grad_rows + grad_resid_b).astype(bf16)
    self_out_rows = lax.dynamic_slice_in_dim(w_self_out, core * half, half, 0)
    grad_mix = dot_nn(self_out_rows, grad_attn_b).astype(bf16)
    g_own = attention_call(*self_args, (self_log, mix_own, grad_mix), 256)
    g_mate = [to_mate(g) for g in g_own]
    mix_near, mix_far = near_far(self_mix)
    attn_halves = grad_attn_b.reshape(2, half, length)
    where = core.astype(jnp.int32).reshape(1)
    grads = (*g_own, *g_mate)
    send = self_products(grads, normed_pieces[1], attn_halves, mix_far, where)
    sum_far, enc_got, send = lax.optimization_barrier((sum_far, enc_got, send))
    side_sum = (side_keep.astype(f32) + side_got.astype(f32)).astype(bf16)
    side_started = dp_start(side_sum.reshape(2, dp_size, block, 2 * depth))
    branch_sum = by_row(
        pick(sum_o, chip) + sum_far[1].astype(f32), pick(sum_t, chip) + sum_far[0].astype(f32)
    )
    new_state = jnp.stack(
        [guess_a + correct[0] * branch_sum, guess_b + correct[1] * branch_sum], axis=1
    ).astype(bf16)
    grad_correct = (jnp.sum(cot_a * branch_sum), jnp.sum(cot_b * branch_sum))
    grad_encoder = by_row(encoder_grad(me), enc_got.astype(f32))
    got = to_peer(send)
    keep = self_products(grads, normed_pieces[0], attn_halves, mix_near, where)
    both_in = into_active(grads, (own_near, mate_near, own_far, mate_far))
    blocks = (2, 2, count, block, 2 * depth)
    side_terms = dp_terms(side_started)
    finished = finish(keep.reshape(blocks), got.reshape(blocks), side_terms, ffn_terms, dp_size)
    both_act = jnp.stack([act_own, act_far]).astype(f32)
    gain_a = norm_gains[0].reshape(4, depth)
    both_gain = jnp.stack([pick(gain_a, me), pick(gain_a, far)])[:, :, None]
    inner = jnp.sum(both_gain * both_in * both_act, axis=(0, 1))[None]
    inner = (inner + to_mate(inner)) / width
    split_b = grad_resid_b.reshape(4, depth, length)
    both_b = jnp.stack([pick(split_b, me), pick(split_b, far)])
    both_back = scale_a * both_gain * both_in - both_act * (scale_a * scale_a * scale_a) * inner
    grad_active = (both_b + both_back).astype(bf16)
    gain_sums = jnp.sum(both_in * both_act * scale_a, axis=2)
    slot = jnp.arange(4, dtype=jnp.int32)[:, None]
    gain_grad_a = (
        jnp.where(slot == me, gain_sums[0][None], 0.0)
        + jnp.where(slot == far, gain_sums[1][None], 0.0)
    ).reshape(width)

    active_got = to_peer(grad_active[1])
    grad_state, late_sums = state_grads(
        predict, chip.astype(jnp.int32).reshape(1), wide_state, cotangent, grad_active[0], active_got
    )
    grad_predict = (
        early_sums[0] + late_sums[0, 0] + late_sums[1, 0],
        early_sums[1] + late_sums[0, 1] + late_sums[1, 1],
        early_sums[2],
        early_sums[3],
    )
    lane = jnp.arange(width, dtype=jnp.int32)
    scalars = sum(
        jnp.where(lane == i, value, 0.0)
        for i, value in enumerate((*grad_predict, grad_correct[0], grad_correct[1]))
    )
    total = all_sum(
        jnp.stack([gain_grad_a, 0.5 * gain_grad_b, 0.5 * gain_grad_c, scalars]), dp_size, 4
    )

    return (
        new_state,
        grad_state,
        grad_encoder,
        *finished,
        total[:3],
        total[3, :4].reshape(2, 2),
        total[3, 4:6],
    )


def choose(paired, dp_size, wide_state, *rest):
    if paired and wide_state.shape[0] == 2:
        return paired_shards(dp_size, wide_state, *rest)
    return shards(wide_state, *rest)


def solution(mesh):
    in_specs = (
        P("dp", None, "mp", None),
        P("dp", "mp", None),
        P("dp", None),
        P("dp", None),
        P(None, "mp", None),
        P("mp", None),
        P(None, "mp", None),
        P("mp", None),
        P(None, None, "mp"),
        P("mp", None),
        P(),
        P(),
        P(),
        P("dp", None, "mp", None),
    )
    out_specs = (
        P("dp", None, "mp", None),
        P("dp", None, "mp", None),
        P("dp", "mp", None),
        P(None, "mp", "dp"),
        P("mp", "dp"),
        P(None, "mp", "dp"),
        P("mp", "dp"),
        P(None, "dp", "mp"),
        P("mp", "dp"),
        P(),
        P(),
        P(),
    )
    paired = mesh.shape["mp"] == 4
    body = functools.partial(choose, paired, mesh.shape["dp"])
    return jax.shard_map(
        body, mesh=mesh, in_specs=in_specs, out_specs=out_specs, check_vma=False
    )
```

```python
import functools

import jax
import jax.numpy as jnp
from jax import lax
from jax.experimental import pallas as pl
from jax.experimental.pallas import tpu as pltpu
from jax.sharding import PartitionSpec as P

HEADS = 12
HEAD = 64


DP, MP = "dp", "mp"
EPSILON = 1e-06
MASKED_SCORE = -1e30


def rms_norm(values, norm_gain):
    mean_sq = jnp.mean(values * values, axis=-1, keepdims=True)
    return values * lax.rsqrt(mean_sq + EPSILON) * norm_gain


def rms_back(values, norm_gain, incoming):
    _, pullback = jax.vjp(rms_norm, values, norm_gain)
    return pullback(incoming)


def gated_unit(gate_pre, up_pre):
    return jax.nn.gelu(gate_pre, approximate=True) * up_pre


def head_split(matrix):
    return matrix.reshape(matrix.shape[0], matrix.shape[1], HEADS, HEAD)


def head_join(tensor):
    return tensor.reshape(tensor.shape[0], tensor.shape[1], HEADS * HEAD)


def self_mask(segments, key_valid, query_start, query_len, key_len):
    seg_query = lax.dynamic_slice_in_dim(segments, query_start, query_len, 1)
    live_key = key_valid > 0
    query_pos = query_start + jnp.arange(query_len, dtype=jnp.int32)
    key_pos = jnp.arange(key_len, dtype=jnp.int32)
    earlier = key_pos[None, None, :] <= query_pos[None, :, None]
    itself = key_pos[None, None, :] == query_pos[None, :, None]
    same_doc = seg_query[:, :, None] == segments[:, None, :]
    return same_doc & earlier & live_key[:, None, :] | itself


def scores_of(queries, key_rows, allowed):
    scores = jnp.einsum(
        "rqhd,rkhd->rhqk",
        head_split(queries),
        head_split(key_rows),
        preferred_element_type=jnp.float32,
    ) * HEAD ** (-0.5)
    if allowed is None:
        return scores
    return jnp.where(allowed[:, None], scores, MASKED_SCORE)


def attend(queries, key_rows, value_rows, allowed):
    scores = scores_of(queries, key_rows, allowed)
    top_score = jnp.max(scores, axis=-1, keepdims=True)
    exponent = jnp.exp(scores - top_score)
    row_total = jnp.sum(exponent, axis=-1, keepdims=True)
    attn_probs = (exponent / row_total).astype(jnp.bfloat16)
    mixed_heads = jnp.einsum(
        "rhqk,rkhd->rqhd", attn_probs, head_split(value_rows), preferred_element_type=jnp.float32
    )
    return (head_join(mixed_heads).astype(jnp.bfloat16), top_score + jnp.log(row_total))


def query_side_grads(queries, key_rows, value_rows, allowed, log_total, grad_mix):
    scores = scores_of(queries, key_rows, allowed)
    attn_probs = jnp.exp(scores - log_total)
    grad_heads = head_split(grad_mix)
    grad_probs = jnp.einsum(
        "rqhd,rkhd->rhqk", grad_heads, head_split(value_rows), preferred_element_type=jnp.float32
    )
    row_dot = jnp.sum(grad_probs * attn_probs, axis=-1, keepdims=True)
    grad_scores = (attn_probs * (grad_probs - row_dot)).astype(jnp.bfloat16)
    grad_query = head_join(
        jnp.einsum(
            "rhqk,rkhd->rqhd", grad_scores, head_split(key_rows), preferred_element_type=jnp.float32
        )
    ) * HEAD ** (-0.5)
    grad_key = head_join(
        jnp.einsum(
            "rhqk,rqhd->rkhd", grad_scores, head_split(queries), preferred_element_type=jnp.float32
        )
    ) * HEAD ** (-0.5)
    grad_value = head_join(
        jnp.einsum(
            "rhqk,rqhd->rkhd",
            attn_probs.astype(jnp.bfloat16),
            grad_heads,
            preferred_element_type=jnp.float32,
        )
    )
    return (grad_query, jnp.stack([grad_key, grad_value]), row_dot)


def shards(
    wide_state,
    encoder,
    segments,
    key_valid,
    self_qkv,
    self_out,
    cross_qkv,
    cross_out,
    ffn_in,
    ffn_out,
    norm_gains,
    predict,
    correct,
    cotangent,
):
    length = segments.shape[1]
    local_len = length // lax.axis_size("mp")
    offset = lax.axis_index(MP) * local_len
    state_f = jnp.transpose(wide_state.astype(jnp.float32), (0, 3, 1, 2))
    block_a = state_f[:, :, 0]
    block_b = state_f[:, :, 1]
    guess_a = predict[0, 0] * block_a + predict[0, 1] * block_b
    guess_b = predict[1, 0] * block_a + predict[1, 1] * block_b
    w_self, w_self_out, w_cross, w_cross_out = (
        lax.all_gather(self_qkv, "mp", axis=1, tiled=True),
        lax.all_gather(self_out, "mp", axis=0, tiled=True),
        lax.all_gather(cross_qkv, "mp", axis=1, tiled=True),
        lax.all_gather(cross_out, "mp", axis=0, tiled=True),
    )
    active = lax.all_to_all(
        guess_a.astype(jnp.bfloat16), "mp", split_axis=1, concat_axis=2, tiled=True
    )
    cross_kv = jnp.einsum(
        "rsd,cde->crse", encoder, w_cross[1:], preferred_element_type=jnp.float32
    ).astype(jnp.bfloat16)
    resid_a = active.astype(jnp.float32)
    normed_a = rms_norm(resid_a, norm_gains[0]).astype(jnp.bfloat16)
    self_proj = jnp.einsum(
        "rtd,cde->crte", normed_a, w_self, preferred_element_type=jnp.float32
    ).astype(jnp.bfloat16)
    queries = self_proj[0]
    all_kv, all_ckv = (
        lax.all_gather(self_proj[1:], "mp", axis=2, tiled=True),
        lax.all_gather(cross_kv, "mp", axis=2, tiled=True),
    )
    allowed = self_mask(segments, key_valid, offset, local_len, length)
    self_mix, self_log = attend(queries, all_kv[0], all_kv[1], allowed)
    attn_out = jnp.einsum("rtd,de->rte", self_mix, w_self_out, preferred_element_type=jnp.float32)
    resid_b = resid_a + attn_out
    normed_b = rms_norm(resid_b, norm_gains[1]).astype(jnp.bfloat16)
    cross_q = jnp.einsum(
        "rtd,de->rte", normed_b, w_cross[0], preferred_element_type=jnp.float32
    ).astype(jnp.bfloat16)
    cross_mix, cross_log = attend(cross_q, all_ckv[0], all_ckv[1], None)
    cross_res = jnp.einsum(
        "rtd,de->rte", cross_mix, w_cross_out, preferred_element_type=jnp.float32
    )
    resid_c = resid_b + cross_res
    normed_c = rms_norm(resid_c, norm_gains[2]).astype(jnp.bfloat16)
    all_normed = lax.all_gather(normed_c, "mp", axis=1, tiled=True)
    gate_up = jnp.einsum("rtd,cdf->crtf", all_normed, ffn_in, preferred_element_type=jnp.float32)
    hidden = gated_unit(gate_up[0], gate_up[1]).astype(jnp.bfloat16)
    ffn_part = jnp.einsum("rtf,fd->rtd", hidden, ffn_out, preferred_element_type=jnp.float32)
    ffn_res = lax.psum_scatter(
        ffn_part.astype(jnp.bfloat16), "mp", scatter_dimension=2, tiled=True
    ).astype(jnp.float32)
    branch_rows = (attn_out + cross_res).astype(jnp.bfloat16)
    branch_cols = lax.all_to_all(branch_rows, "mp", split_axis=2, concat_axis=1, tiled=True)
    branch_sum = branch_cols.astype(jnp.float32) + ffn_res
    new_rows = jnp.stack(
        [guess_a + correct[0] * branch_sum, guess_b + correct[1] * branch_sum], axis=2
    )
    new_state = jnp.transpose(new_rows, (0, 2, 3, 1)).astype(jnp.bfloat16)
    cot_f = jnp.transpose(cotangent.astype(jnp.float32), (0, 3, 1, 2))
    cot_a = cot_f[:, :, 0]
    cot_b = cot_f[:, :, 1]
    grad_branch = (correct[0] * cot_a + correct[1] * cot_b).astype(jnp.bfloat16)
    grad_correct = jnp.stack([jnp.sum(cot_a * branch_sum), jnp.sum(cot_b * branch_sum)])
    all_grad = lax.all_gather(grad_branch, "mp", axis=2, tiled=True)
    grad_rows = lax.dynamic_slice_in_dim(all_grad, offset, local_len, 1).astype(jnp.float32)
    grad_hidden = jnp.einsum("rtd,fd->rtf", all_grad, ffn_out, preferred_element_type=jnp.float32)
    grad_ffn_out = jnp.einsum("rtf,rtd->fd", hidden, all_grad, preferred_element_type=jnp.float32)
    _, gate_back = jax.vjp(gated_unit, gate_up[0], gate_up[1])
    grad_gate, grad_up = gate_back(grad_hidden)
    grad_gate_up = jnp.stack([grad_gate, grad_up]).astype(jnp.bfloat16)
    grad_ffn_in = jnp.einsum(
        "rtd,crtf->cdf", all_normed, grad_gate_up, preferred_element_type=jnp.float32
    )
    normed_part = jnp.einsum(
        "crtf,cdf->rtd", grad_gate_up, ffn_in, preferred_element_type=jnp.float32
    )
    grad_normed_c = lax.psum_scatter(normed_part, "mp", scatter_dimension=1, tiled=True)
    grad_resid_c, gain_grad_c = rms_back(resid_c, norm_gains[2], grad_normed_c)
    grad_cross_b = (grad_rows + grad_resid_c).astype(jnp.bfloat16)
    grad_cross_out = jnp.einsum(
        "rtd,rte->de", cross_mix, grad_cross_b, preferred_element_type=jnp.float32
    )
    grad_cross_mix = jnp.einsum(
        "rte,de->rtd", grad_cross_b, w_cross_out, preferred_element_type=jnp.float32
    ).astype(jnp.bfloat16)
    grad_cq, cross_key_part, _ = query_side_grads(
        cross_q, all_ckv[0], all_ckv[1], None, cross_log, grad_cross_mix
    )
    grad_cq_b = grad_cq.astype(jnp.bfloat16)
    grad_cross_first = jnp.einsum(
        "rtd,rte->de", normed_b, grad_cq_b, preferred_element_type=jnp.float32
    )
    grad_normed_b = jnp.einsum(
        "rte,de->rtd", grad_cq_b, w_cross[0], preferred_element_type=jnp.float32
    )
    resid_b_part, gain_grad_b = rms_back(resid_b, norm_gains[1], grad_normed_b)
    grad_resid_b = grad_resid_c + resid_b_part
    grad_attn_b = (grad_rows + grad_resid_b).astype(jnp.bfloat16)
    grad_self_out = jnp.einsum(
        "rtd,rte->de", self_mix, grad_attn_b, preferred_element_type=jnp.float32
    )
    grad_self_mix = jnp.einsum(
        "rte,de->rtd", grad_attn_b, w_self_out, preferred_element_type=jnp.float32
    ).astype(jnp.bfloat16)
    grad_query, self_key_part, _ = query_side_grads(
        queries, all_kv[0], all_kv[1], allowed, self_log, grad_self_mix
    )
    own_kv, own_ckv = (
        lax.psum_scatter(
            self_key_part.astype(jnp.bfloat16), "mp", scatter_dimension=2, tiled=True
        ).astype(jnp.float32),
        lax.psum_scatter(
            cross_key_part.astype(jnp.bfloat16), "mp", scatter_dimension=2, tiled=True
        ).astype(jnp.float32),
    )
    own_kv_b = own_kv.astype(jnp.bfloat16)
    own_ckv_b = own_ckv.astype(jnp.bfloat16)
    grad_qkv_b = jnp.concatenate([grad_query.astype(jnp.bfloat16)[None], own_kv_b], axis=0)
    grad_self_qkv = jnp.einsum(
        "rtd,crte->cde", normed_a, grad_qkv_b, preferred_element_type=jnp.float32
    )
    grad_normed_a = jnp.einsum(
        "crte,cde->rtd", grad_qkv_b, w_self, preferred_element_type=jnp.float32
    )
    grad_cross_kv = jnp.einsum(
        "rsd,crse->cde", encoder, own_ckv_b, preferred_element_type=jnp.float32
    )
    grad_encoder = jnp.einsum(
        "crse,cde->rsd", own_ckv_b, w_cross[1:], preferred_element_type=jnp.float32
    )
    grad_cross_qkv = jnp.concatenate([grad_cross_first[None], grad_cross_kv], axis=0)
    resid_a_part, gain_grad_a = rms_back(resid_a, norm_gains[0], grad_normed_a)
    grad_active = (grad_resid_b + resid_a_part).astype(jnp.bfloat16)
    grad_cols = lax.all_to_all(grad_active, "mp", split_axis=2, concat_axis=1, tiled=True).astype(
        jnp.float32
    )
    grad_guess_a = cot_a + grad_cols
    grad_predict = jnp.stack(
        [
            jnp.stack([jnp.sum(grad_guess_a * block_a), jnp.sum(grad_guess_a * block_b)]),
            jnp.stack([jnp.sum(cot_b * block_a), jnp.sum(cot_b * block_b)]),
        ]
    )
    grad_rows_state = jnp.stack(
        [
            predict[0, 0] * grad_guess_a + predict[1, 0] * cot_b,
            predict[0, 1] * grad_guess_a + predict[1, 1] * cot_b,
        ],
        axis=2,
    )
    grad_state = jnp.transpose(grad_rows_state, (0, 2, 3, 1))
    gain_grads = jnp.stack([gain_grad_a, gain_grad_b, gain_grad_c])
    part_self_qkv, part_self_out, part_cross_qkv, part_cross_out, part_ffn_in, part_ffn_out = (
        lax.psum_scatter(
            grad_self_qkv.astype(jnp.bfloat16), "dp", scatter_dimension=2, tiled=True
        ).astype(jnp.float32),
        lax.psum_scatter(
            grad_self_out.astype(jnp.bfloat16), "dp", scatter_dimension=1, tiled=True
        ).astype(jnp.float32),
        lax.psum_scatter(
            grad_cross_qkv.astype(jnp.bfloat16), "dp", scatter_dimension=2, tiled=True
        ).astype(jnp.float32),
        lax.psum_scatter(
            grad_cross_out.astype(jnp.bfloat16), "dp", scatter_dimension=1, tiled=True
        ).astype(jnp.float32),
        lax.psum_scatter(
            grad_ffn_in.astype(jnp.bfloat16), "dp", scatter_dimension=1, tiled=True
        ).astype(jnp.float32),
        lax.psum_scatter(
            grad_ffn_out.astype(jnp.bfloat16), "dp", scatter_dimension=1, tiled=True
        ).astype(jnp.float32),
    )
    final_self_qkv, final_self_out, final_cross_qkv, final_cross_out = (
        lax.psum_scatter(
            part_self_qkv.astype(jnp.bfloat16), "mp", scatter_dimension=1, tiled=True
        ).astype(jnp.float32),
        lax.psum_scatter(
            part_self_out.astype(jnp.bfloat16), "mp", scatter_dimension=0, tiled=True
        ).astype(jnp.float32),
        lax.psum_scatter(
            part_cross_qkv.astype(jnp.bfloat16), "mp", scatter_dimension=1, tiled=True
        ).astype(jnp.float32),
        lax.psum_scatter(
            part_cross_out.astype(jnp.bfloat16), "mp", scatter_dimension=0, tiled=True
        ).astype(jnp.float32),
    )
    total_gains, total_predict, total_correct = lax.psum(
        (gain_grads, grad_predict, grad_correct), ("dp", "mp")
    )
    return (
        new_state,
        grad_state,
        grad_encoder,
        final_self_qkv,
        final_self_out,
        final_cross_qkv,
        final_cross_out,
        part_ffn_in,
        part_ffn_out,
        total_gains,
        total_predict,
        total_correct,
    )


def dot_tn(left, right):
    return lax.dot_general(
        left, right, (((0,), (0,)), ((), ())), preferred_element_type=jnp.float32
    )


def dot_nn(left, right):
    return lax.dot_general(
        left, right, (((1,), (0,)), ((), ())), preferred_element_type=jnp.float32
    )


def dot_nt(left, right):
    return lax.dot_general(
        left, right, (((1,), (1,)), ((), ())), preferred_element_type=jnp.float32
    )


def block_scores(keys_t, query, seg_ref, code_ref, block, size, high):
    scores = dot_nn(keys_t[:high], query)
    if seg_ref is None:
        return scores
    seg_query = seg_ref[:, block * size : (block + 1) * size]
    codes = jnp.concatenate([code_ref[:high, :]] * (size // 128), axis=1)
    same = codes == seg_query
    low = block * size
    key = lax.broadcasted_iota(jnp.int32, (size, size), 0)
    query_pos = lax.broadcasted_iota(jnp.int32, (size, size), 1)
    near = (same[low:] & (key <= query_pos)) | (key == query_pos)
    lower = jnp.where(near, scores[low:], MASKED_SCORE)
    if low == 0:
        return lower
    return jnp.concatenate([jnp.where(same[:low], scores[:low], MASKED_SCORE), lower], axis=0)


def attend_kernel(masked, size, *refs):
    if masked:
        q_ref, k_ref, v_ref, seg_ref, code_ref, mix_ref, log_ref = refs
    else:
        q_ref, k_ref, v_ref, mix_ref, log_ref = refs
        seg_ref = code_ref = None
    key_len, query_len = k_ref.shape[1], q_ref.shape[1]
    keys_t = k_ref[...].T
    values = v_ref[...]
    for block in range(query_len // size):
        cols = slice(block * size, (block + 1) * size)
        high = (block + 1) * size if masked else key_len
        query = q_ref[:, cols] * jnp.bfloat16(HEAD ** (-0.5))
        scores = block_scores(keys_t, query, seg_ref, code_ref, block, size, high)
        top = jnp.max(scores, axis=0, keepdims=True)
        exponent = jnp.exp(scores - top)
        total = jnp.sum(exponent, axis=0, keepdims=True)
        mixed = dot_nn(values[:, :high], exponent.astype(jnp.bfloat16))
        mix_ref[:, cols] = (mixed / total).astype(jnp.bfloat16)
        log_ref[0, :, cols] = top + jnp.log(total)


def attend_back_kernel(masked, size, *refs):
    if masked:
        q_ref, k_ref, v_ref, seg_ref, code_ref = refs[:5]
        refs = refs[5:]
    else:
        q_ref, k_ref, v_ref = refs[:3]
        seg_ref = code_ref = None
        refs = refs[3:]
    log_ref, mix_ref, grad_ref, dq_ref, dk_ref, dv_ref, dk_sum, dv_sum = refs
    key_len, query_len = k_ref.shape[1], q_ref.shape[1]
    keys = k_ref[...]
    keys_t = keys.T
    values_t = v_ref[...].T
    last = query_len // size - 1
    for block in range(last, -1, -1):
        cols = slice(block * size, (block + 1) * size)
        high = (block + 1) * size if masked else key_len
        query = q_ref[:, cols] * jnp.bfloat16(HEAD ** (-0.5))
        grad = grad_ref[:, cols]
        scores = block_scores(keys_t, query, seg_ref, code_ref, block, size, high)
        probs = jnp.exp(scores - log_ref[0, :, cols])
        grad_probs = dot_nn(values_t[:high], grad)
        row_dot = jnp.sum(
            grad.astype(jnp.float32) * mix_ref[:, cols].astype(jnp.float32), axis=0, keepdims=True
        )
        grad_scores = (probs * (grad_probs - row_dot)).astype(jnp.bfloat16)
        dq_ref[:, cols] = (dot_nn(keys[:, :high], grad_scores) * HEAD ** (-0.5)).astype(
            jnp.bfloat16
        )
        dk = dot_nt(query, grad_scores)
        dv = dot_nt(grad, probs.astype(jnp.bfloat16))
        if block == last:
            dk_sum[:, :high] = dk
            dv_sum[:, :high] = dv
        else:
            dk_sum[:, :high] += dk
            dv_sum[:, :high] += dv
    dk_ref[...] = dk_sum[...].astype(jnp.bfloat16)
    dv_ref[...] = dv_sum[...].astype(jnp.bfloat16)


def head_rows(first, length):
    return pl.BlockSpec((HEAD, length), lambda head: (first + head, 0))


def attention_call(queries, keys, values, heads, mask, back, size):
    (q_arr, q_at), (k_arr, k_at), (v_arr, v_at) = queries, keys, values
    q_len, k_len = q_arr.shape[1], k_arr.shape[1]
    operands = [q_arr, k_arr, v_arr]
    specs = [head_rows(q_at, q_len), head_rows(k_at, k_len), head_rows(v_at, k_len)]
    if mask is not None:
        operands += list(mask)
        specs += [
            pl.BlockSpec((1, q_len), lambda head: (0, 0)),
            pl.BlockSpec((k_len, 128), lambda head: (0, 0)),
        ]
    log_spec = pl.BlockSpec((1, 1, q_len), lambda head: (head, 0, 0))
    q_out = jax.ShapeDtypeStruct((heads * HEAD, q_len), jnp.bfloat16)
    k_out = jax.ShapeDtypeStruct((heads * HEAD, k_len), jnp.bfloat16)
    pairs = heads * q_len * k_len * (0.6 if mask is not None else 1.0)
    if back is None:
        kernel, dots, scratch = attend_kernel, 2, []
        out_shape = [q_out, jax.ShapeDtypeStruct((heads, 1, q_len), jnp.float32)]
        out_specs = [head_rows(0, q_len), log_spec]
    else:
        kernel, dots = attend_back_kernel, 5
        operands += list(back)
        specs += [log_spec, head_rows(0, q_len), head_rows(0, q_len)]
        out_shape = [q_out, k_out, k_out]
        out_specs = [head_rows(0, q_len), head_rows(0, k_len), head_rows(0, k_len)]
        scratch = [pltpu.VMEM((HEAD, k_len), jnp.float32)] * 2
    return pl.pallas_call(
        functools.partial(kernel, mask is not None, size),
        grid=(heads,),
        in_specs=specs,
        out_specs=out_specs,
        out_shape=out_shape,
        scratch_shapes=scratch,
        compiler_params=pltpu.CompilerParams(vmem_limit_bytes=32 << 20),
        cost_estimate=pl.CostEstimate(
            flops=int(8 * HEAD * dots * pairs),
            bytes_accessed=4 * heads * HEAD * (q_len + k_len) * dots // 2,
            transcendentals=int(pairs),
        ),
        name="attend" if back is None else "attend_back",
    )(*operands)


MESH = pl.DeviceIdType.MESH


def after(value, *earlier):
    return lax.optimization_barrier((value, *earlier))[0]


def rms_scale(values):
    return lax.rsqrt(jnp.mean(values * values, axis=0, keepdims=True) + EPSILON)


def pick(array, index, axis=0):
    return lax.dynamic_index_in_dim(array, index, axis, keepdims=False)


def all_sum_kernel(dp_size, mp_size, *refs):
    early_refs, (late_ref, gains_ref, out_ref) = refs[:6], refs[6:9]
    part_ref, mp_slots, row_sum, dp_slots, mp_send, mp_recv, dp_send, dp_recv = refs[9:]
    late = [late_ref[0, j] + late_ref[1, j] for j in range(2)]
    scalars = [ref[0, 0] + (late[i] if i < 2 else 0.0) for i, ref in enumerate(early_refs)]
    lane = lax.broadcasted_iota(jnp.int32, (1, part_ref.shape[1]), 1)
    part_ref[:3, :] = gains_ref[...]
    part_ref[3:, :] = sum(jnp.where(lane == i, value, 0.0) for i, value in enumerate(scalars))
    dp, mp = lax.axis_index(DP), lax.axis_index(MP)
    mp_peers = [lax.rem(mp + s, mp_size) for s in range(1, mp_size)]
    dp_peers = [lax.rem(dp + s, dp_size) for s in range(1, dp_size)]
    barrier = pltpu.get_barrier_semaphore()
    for peer in mp_peers:
        pl.semaphore_signal(barrier, inc=1, device_id=(dp, peer), device_id_type=MESH)
    for peer in dp_peers:
        pl.semaphore_signal(barrier, inc=1, device_id=(peer, mp), device_id_type=MESH)
    pl.semaphore_wait(barrier, mp_size + dp_size - 2)

    def exchange(source, slots, send, recv, targets):
        copies = []
        for step, target in enumerate(targets):
            copies.append(
                pltpu.make_async_remote_copy(
                    src_ref=source,
                    dst_ref=slots.at[step],
                    send_sem=send.at[step],
                    recv_sem=recv.at[step],
                    device_id=target,
                    device_id_type=MESH,
                )
            )
            copies[-1].start()
        for copy in copies:
            copy.wait()

    exchange(part_ref, mp_slots, mp_send, mp_recv, [(dp, p) for p in mp_peers])
    row_sum[...] = ordered_sum(part_ref, mp_slots, mp, mp_size)
    exchange(row_sum, dp_slots, dp_send, dp_recv, [(p, mp) for p in dp_peers])
    out_ref[...] = ordered_sum(row_sum, dp_slots, dp, dp_size)


def ordered_sum(own_ref, slots, place, size):
    total = jnp.zeros_like(own_ref)
    for device in range(size):
        term = own_ref[...]
        for step in range(size - 1):
            from_here = lax.rem(place + size - step - 1, size) == device
            term = jnp.where(from_here, slots[step], term)
        total += term
    return total


def all_sum(early, late, gains, dp_size, mp_size):
    whole = pl.BlockSpec(memory_space=pltpu.VMEM)
    smem = pl.BlockSpec(memory_space=pltpu.SMEM)
    shape = (4, gains.shape[1])
    return pl.pallas_call(
        functools.partial(all_sum_kernel, dp_size, mp_size),
        out_shape=jax.ShapeDtypeStruct(shape, gains.dtype),
        in_specs=[smem] * 7 + [whole],
        out_specs=whole,
        scratch_shapes=[
            pltpu.VMEM(shape, gains.dtype),
            pltpu.VMEM((mp_size - 1, *shape), gains.dtype),
            pltpu.VMEM(shape, gains.dtype),
            pltpu.VMEM((dp_size - 1, *shape), gains.dtype),
            pltpu.SemaphoreType.DMA((mp_size - 1,)),
            pltpu.SemaphoreType.DMA((mp_size - 1,)),
            pltpu.SemaphoreType.DMA((dp_size - 1,)),
            pltpu.SemaphoreType.DMA((dp_size - 1,)),
        ],
        compiler_params=pltpu.CompilerParams(collective_id=0, has_side_effects=True),
        name="all_sum",
    )(*[value.reshape(1, 1) for value in early], late, gains)


def finish_kernel(dp_size, keep_ref, got_ref, *refs):
    terms = refs[:8]
    qkv_out, out_out, cross_out, cross_out_out, in_out, down_out = refs[8:14]
    step_send, step_land, far_send, far_land = refs[14:18]
    step_sems, far_sems = refs[18:20], refs[20:22]
    side_terms, ffn_terms, load_sem = refs[22:]
    loads = []
    for i, ref in enumerate(terms):
        place = side_terms.at[i] if i < 4 else ffn_terms.at[i - 4]
        loads.append(pltpu.make_async_copy(ref, place, load_sem.at[i]))
        loads[i].start()
    bf16, f32 = jnp.bfloat16, jnp.float32
    dp, mp = lax.axis_index(DP), lax.axis_index(MP)
    core = lax.rem(mp, 2)
    outer, inner = dp // 2, lax.rem(dp, 2)
    count = dp_size // 2
    mate = (outer * 2 + 1 - inner, mp)
    offsets = [(count // 2 + i) % count for i in range(count)]
    offsets = [o for o in offsets if o] + [0]
    places = [lax.rem(outer + o, count) for o in offsets]
    targets = [(place * 2 + inner, mp) for place in places]
    last = count - 1

    barrier = pltpu.get_barrier_semaphore()
    for device in [mate] + targets[:last]:
        pl.semaphore_signal(barrier, inc=1, device_id=device, device_id_type=MESH)
    pl.semaphore_wait(barrier, count)

    def remote(source, target, sems, index, device):
        return pltpu.make_async_remote_copy(
            src_ref=source,
            dst_ref=target,
            send_sem=sems[0].at[index],
            recv_sem=sems[1].at[index],
            device_id=device,
            device_id_type=MESH,
        )

    def summed(place, own):
        index = place * 2 + (inner if own else 1 - inner)
        part, block = lax.rem(index // count + core, 2), lax.rem(index, count)
        return keep_ref[part, :, block].astype(f32) + got_ref[part, :, block].astype(f32)

    stepping = []
    for k, place in enumerate(places):
        step_send[k] = summed(place, False).astype(bf16)
        stepping.append(remote(step_send.at[k], step_land.at[k], step_sems, k, mate))
        stepping[k].start()

    def turned(pairs, first, second):
        depth = first.shape[1]
        for pair in range(2):
            flipped = pairs[pair].T
            for side in range(2):
                mat = 2 * pair + side
                piece = flipped[side * depth : (side + 1) * depth]
                if mat < 3:
                    first[mat] = piece
                else:
                    second[...] = piece

    for load in loads:
        load.wait()
    turned(sum(side_terms[i].astype(f32) for i in range(4)), cross_out, cross_out_out)
    for mat in range(2):
        in_out[mat] = sum(ffn_terms[i, mat].astype(f32) for i in range(4))
    down_out[...] = sum(ffn_terms[i, 2].astype(f32) for i in range(4)).T

    going = []
    for k, place in enumerate(places):
        stepping[k].wait()
        total = summed(place, True) + step_land[k].astype(f32)
        if k == last:
            continue
        far_send[k] = total.astype(bf16)
        going.append(remote(far_send.at[k], far_land.at[k], far_sems, k, targets[k]))
        going[k].start()
    for k, copy in enumerate(going):
        copy.wait()
        total += far_land[k].astype(f32)
    turned(total, qkv_out, out_out)


def finish(keep, got, side_terms, ffn_terms, dp_size):
    pairs, _, rows, columns = keep.shape[1:]
    depth, width = columns // 2, ffn_terms[0].shape[2]
    block = (pairs, rows, columns)
    count = dp_size // 2
    whole = pl.BlockSpec(memory_space=pltpu.VMEM)
    dma = pltpu.SemaphoreType.DMA
    three, one = (3, depth, rows), (depth, rows)
    shapes = [three, one, three, one, (2, rows, width), (width, rows)]
    return pl.pallas_call(
        functools.partial(finish_kernel, dp_size),
        out_shape=[jax.ShapeDtypeStruct(shape, jnp.float32) for shape in shapes],
        in_specs=[whole] * 2 + [pl.BlockSpec(memory_space=pl.ANY)] * 8,
        out_specs=[whole] * 6,
        scratch_shapes=[
            pltpu.VMEM((count, *block), jnp.bfloat16),
            pltpu.VMEM((count, *block), jnp.bfloat16),
            pltpu.VMEM((count - 1, *block), jnp.bfloat16),
            pltpu.VMEM((count - 1, *block), jnp.bfloat16),
            dma((count,)),
            dma((count,)),
            dma((count - 1,)),
            dma((count - 1,)),
            pltpu.VMEM((4, *side_terms[0].shape), jnp.bfloat16),
            pltpu.VMEM((4, *ffn_terms[0].shape), jnp.bfloat16),
            dma((8,)),
        ],
        compiler_params=pltpu.CompilerParams(
            collective_id=1, has_side_effects=True, vmem_limit_bytes=40 << 20
        ),
        name="finish",
    )(keep, got, *side_terms, *ffn_terms)


def join_norm_kernel(place_ref, gain_ref, *refs):
    pieces, (active_ref, normed_ref, scale_ref) = refs[:4], refs[4:]
    depth = pieces[0].shape[0]
    squares = sum(
        jnp.sum(jnp.square(p[...].astype(jnp.float32)), axis=0, keepdims=True) for p in pieces
    )
    scale = lax.rsqrt(squares * (1.0 / (4 * depth)) + EPSILON)
    scale_ref[...] = scale
    for i, piece in enumerate(pieces):
        quarter = place_ref[i]
        value = piece[...]
        active_ref[quarter] = value
        normed = value.astype(jnp.float32) * scale * gain_ref[quarter]
        normed_ref[i] = normed.astype(jnp.bfloat16)


def join_norm(places, gain, pieces):
    depth, length = pieces[0].shape
    whole = pl.BlockSpec(memory_space=pltpu.VMEM)
    full = jax.ShapeDtypeStruct((4, depth, length), jnp.bfloat16)
    return pl.pallas_call(
        join_norm_kernel,
        out_shape=[full, full, jax.ShapeDtypeStruct((1, length), jnp.float32)],
        in_specs=[pl.BlockSpec(memory_space=pltpu.SMEM)] + [whole] * 5,
        out_specs=[whole] * 3,
        cost_estimate=pl.CostEstimate(
            flops=40 * depth * length, bytes_accessed=24 * depth * length, transcendentals=length
        ),
        name="join_norm",
    )(places, gain, *pieces)


def dot_tt(left, right):
    return lax.dot_general(
        left, right, (((0,), (1,)), ((), ())), preferred_element_type=jnp.float32
    )


def outer_kernel(sizes, *refs):
    keep_ref, send_ref = refs[-2:]
    depth = refs[0].shape[0]
    at, mat = 0, 0
    for size in sizes:
        near, far = refs[at][...], refs[at + 1][...]
        for ref in refs[at + 2 : at + 2 + size]:
            columns = slice(mat % 2 * depth, (mat % 2 + 1) * depth)
            for low in range(0, ref.shape[0], 384):
                block = ref[low : low + 384, :]
                rows = slice(low, low + block.shape[0])
                keep_ref[mat // 2, rows, columns] = dot_nt(block, near).astype(jnp.bfloat16)
                send_ref[mat // 2, rows, columns] = dot_nt(block, far).astype(jnp.bfloat16)
            mat += 1
        at += 2 + size


def outer_products(groups):
    operands, sizes, flops = [], [], 0
    for outer, inner in groups:
        operands += [*inner, *outer]
        sizes.append(len(outer))
        flops += sum(4 * o.size * inner[0].shape[0] for o in outer)
    rows, columns = groups[0][0][0].shape[0], 2 * operands[0].shape[0]
    whole = pl.BlockSpec(memory_space=pltpu.VMEM)
    shape = jax.ShapeDtypeStruct((sum(sizes) // 2, rows, columns), jnp.bfloat16)
    return pl.pallas_call(
        functools.partial(outer_kernel, tuple(sizes)),
        out_shape=[shape, shape],
        in_specs=[whole] * len(operands),
        out_specs=[whole] * 2,
        compiler_params=pltpu.CompilerParams(vmem_limit_bytes=32 << 20),
        cost_estimate=pl.CostEstimate(
            flops=flops,
            bytes_accessed=sum(2 * o.size for o in operands) + 4 * shape.size,
            transcendentals=0,
        ),
        name="outer_products",
    )(*operands)


def self_products_kernel(core_ref, *refs):
    grads, (norm_ref, attn_ref, mix_ref, out_ref) = refs[:6], refs[6:]
    core = core_ref[0]
    depth = norm_ref.shape[0]
    norm, mix = norm_ref[...], mix_ref[...]
    for side in range(2):
        grad_rows = [ref[...] for ref in grads[3 * side : 3 * side + 3]]
        grad_rows.append(attn_ref[core if side == 0 else 1 - core])
        for mat, grad in enumerate(grad_rows):
            columns = slice(mat % 2 * depth, (mat % 2 + 1) * depth)
            value = dot_nt(grad, mix if mat == 3 else norm)
            out_ref[side, mat // 2, :, columns] = value.astype(jnp.bfloat16)


def self_products(grads, normed, grad_attn, mix, core):
    half, length = grads[0].shape
    depth = normed.shape[0]
    whole = pl.BlockSpec(memory_space=pltpu.VMEM)
    operands = [*grads, normed, grad_attn, mix]
    shape = jax.ShapeDtypeStruct((2, 2, half, 2 * depth), jnp.bfloat16)
    return pl.pallas_call(
        self_products_kernel,
        out_shape=shape,
        in_specs=[pl.BlockSpec(memory_space=pltpu.SMEM)] + [whole] * len(operands),
        out_specs=whole,
        compiler_params=pltpu.CompilerParams(vmem_limit_bytes=32 << 20),
        cost_estimate=pl.CostEstimate(
            flops=16 * half * length * depth,
            bytes_accessed=sum(2 * o.size for o in operands) + 2 * shape.size,
            transcendentals=0,
        ),
        name="self_products",
    )(core, *operands)


def into_kernel(*refs):
    grads, (near_own, near_mate, far_own, far_mate, into_ref) = refs[:6], refs[6:]
    for mat in range(3):
        joined = jnp.concatenate([grads[mat][...], grads[3 + mat][...]], axis=0)
        for out, (own, mate) in enumerate(((near_own, near_mate), (far_own, far_mate))):
            term = dot_nn(jnp.concatenate([own[mat], mate[mat]], axis=1), joined)
            if mat == 0:
                into_ref[out] = term
            else:
                into_ref[out] += term


def into_active(grads, weights):
    half, length = grads[0].shape
    depth = weights[0].shape[1]
    whole = pl.BlockSpec(memory_space=pltpu.VMEM)
    operands = [*grads, *weights]
    return pl.pallas_call(
        into_kernel,
        out_shape=jax.ShapeDtypeStruct((2, depth, length), jnp.float32),
        in_specs=[whole] * len(operands),
        out_specs=whole,
        compiler_params=pltpu.CompilerParams(vmem_limit_bytes=32 << 20),
        cost_estimate=pl.CostEstimate(
            flops=24 * half * length * depth,
            bytes_accessed=sum(2 * o.size for o in operands) + 8 * depth * length,
            transcendentals=0,
        ),
        name="into_active",
    )(*operands)


def state_grads_kernel(predict_ref, chip_ref, state_ref, cot_ref, own_ref, far_ref, out_ref, sum_ref):
    row = pl.program_id(0)
    own_row = row == chip_ref[0]
    grad = jnp.where(own_row, own_ref[...], far_ref[...]).astype(jnp.float32)
    for j in range(2):
        sum_ref[row, j] = jnp.sum(grad * state_ref[0, j].astype(jnp.float32))
    guess_a = cot_ref[0, 0].astype(jnp.float32) + grad
    guess_b = cot_ref[0, 1].astype(jnp.float32)
    for j in range(2):
        out_ref[0, j] = predict_ref[0, j] * guess_a + predict_ref[1, j] * guess_b


def state_grads(predict, chip, wide_state, cotangent, own, far):
    rows, blocks, depth, length = wide_state.shape
    smem = pl.BlockSpec(memory_space=pltpu.SMEM)
    one_row = pl.BlockSpec((1, blocks, depth, length), lambda row: (row, 0, 0, 0))
    whole = pl.BlockSpec((depth, length), lambda row: (0, 0))
    return pl.pallas_call(
        state_grads_kernel,
        grid=(rows,),
        out_shape=[
            jax.ShapeDtypeStruct(wide_state.shape, jnp.float32),
            jax.ShapeDtypeStruct((rows, blocks), jnp.float32),
        ],
        in_specs=[smem, smem, one_row, one_row, whole, whole],
        out_specs=[one_row, smem],
        compiler_params=pltpu.CompilerParams(vmem_limit_bytes=32 << 20),
        cost_estimate=pl.CostEstimate(
            flops=12 * wide_state.size, bytes_accessed=9 * wide_state.size, transcendentals=0
        ),
        name="state_grads",
    )(predict, chip, wide_state, cotangent, own, far)


def paired_shards(
    dp_size,
    wide_state,
    encoder,
    segments,
    key_valid,
    self_qkv,
    self_out,
    cross_qkv,
    cross_out,
    ffn_in,
    ffn_out,
    norm_gains,
    predict,
    correct,
    cotangent,
):
    bf16, f32 = jnp.bfloat16, jnp.float32
    me = lax.axis_index(MP)
    chip, core = me // 2, me % 2
    far = me ^ 2
    mates = [(i, i ^ 1) for i in range(4)]
    peers = [(i, i ^ 2) for i in range(4)]

    def to_mate(array):
        return lax.ppermute(array, MP, mates)

    def to_peer(array):
        return lax.ppermute(array, MP, peers)

    def quarters(own, across, axis=0):
        pieces = [own, across, to_mate(own), to_mate(across)]
        stacked = jnp.stack(pieces)
        order = [pick(stacked, ((j % 2) ^ core) * 2 + ((j // 2) ^ chip)) for j in range(4)]
        return jnp.concatenate(order, axis=axis)

    def halves(own, axis=0):
        other = to_mate(own)
        return jnp.where(
            core == 0,
            jnp.concatenate([own, other], axis=axis),
            jnp.concatenate([other, own], axis=axis),
        )

    def by_row(own, other):
        return jnp.where(chip == 0, jnp.stack([own, other]), jnp.stack([other, own]))

    def project(weights, values):
        return dot_tn(weights, values)

    length = wide_state.shape[3]
    width = self_qkv.shape[2]
    depth = self_qkv.shape[1]
    half = width // 2
    heads = half // HEAD
    gains = norm_gains[:, :, None]

    block_a = wide_state[:, 0].astype(f32)
    block_b = wide_state[:, 1].astype(f32)
    guess_a = predict[0, 0] * block_a + predict[0, 1] * block_b
    guess_b = predict[1, 0] * block_a + predict[1, 1] * block_b
    active_rows = guess_a.astype(bf16)
    act_own = pick(active_rows, chip)
    act_far = to_peer(pick(active_rows, 1 - chip))
    qkv_far = to_peer(self_qkv)
    cot_a = cotangent[:, 0].astype(f32)
    cot_b = cotangent[:, 1].astype(f32)
    grad_branch = (correct[0] * cot_a + correct[1] * cot_b).astype(bf16)
    early_sums = [jnp.sum(c * b) for c in (cot_a, cot_b) for b in (block_a, block_b)]
    seg_row = pick(segments, chip)
    code = jnp.where(pick(key_valid, chip) > 0, seg_row, -1)
    mask = (seg_row[None], jnp.broadcast_to(code[:, None], (wide_state.shape[3], 128)))
    act_far, grad_branch, early_sums, mask = lax.optimization_barrier(
        (act_far, grad_branch, early_sums, mask)
    )
    act_pieces = [act_own, act_far, to_mate(act_own), to_mate(act_far)]
    places = jnp.stack([me, far, me ^ 1, me ^ 3]).astype(jnp.int32)
    active, normed_pieces, scale_a = join_norm(
        places, norm_gains[0].reshape(4, depth, 1), act_pieces
    )
    active = active.reshape(width, length)
    normed_a = normed_pieces.reshape(width, length)
    self_out_far = to_peer(self_out)
    enc_far = to_peer(pick(encoder, 1 - chip))
    cross_qkv_far = to_peer(cross_qkv)
    cross_out_far = to_peer(cross_out)
    grad_far = to_peer(grad_branch)

    def columns(array, which):
        return lax.dynamic_slice_in_dim(array, which * half, half, array.ndim - 1)

    own_near, own_far = columns(self_qkv, core), columns(qkv_far, core)
    mate_near, mate_far = columns(self_qkv, 1 - core), columns(qkv_far, 1 - core)
    w_qkv = jnp.concatenate([own_near, own_far, to_mate(mate_near), to_mate(mate_far)], axis=1)
    w_self_out = quarters(self_out, self_out_far)
    enc = quarters(pick(encoder, chip), enc_far)
    w_cross = quarters(cross_qkv, cross_qkv_far, axis=1)
    w_cross_out = quarters(cross_out, cross_out_far)
    all_grad = quarters(grad_branch, grad_far, axis=1)
    grad_own = pick(all_grad, chip)
    grad_other = pick(all_grad, 1 - chip)

    resid_a = active.astype(f32)
    qkv = jnp.concatenate([project(w_qkv[i], normed_a).astype(bf16) for i in range(3)], axis=0)
    self_args = ((qkv, 0), (qkv, heads), (qkv, 2 * heads), heads, mask)
    mix_own, self_log = attention_call(*self_args, None, 512)
    self_mix = halves(mix_own)
    attn_out = project(w_self_out, self_mix)

    resid_b = resid_a + attn_out
    scale_b = rms_scale(resid_b)
    normed_b = (resid_b * scale_b * gains[1]).astype(bf16)
    w_cross_own = columns(w_cross, core)
    cross_q = project(w_cross_own[0], normed_b).astype(bf16)
    cross_kv = jnp.concatenate(
        [
            lax.dot_general(
                w_cross_own[i], enc, (((0,), (1,)), ((), ())), preferred_element_type=f32
            ).astype(bf16)
            for i in (1, 2)
        ],
        axis=0,
    )
    cross_args = ((cross_q, 0), (cross_kv, 0), (cross_kv, heads), heads, None)
    cmix_own, cross_log = attention_call(*cross_args, None, 512)
    cross_mix = halves(cmix_own)
    cross_res = project(w_cross_out, cross_mix)
    resid_c = resid_b + cross_res
    scale_c = rms_scale(resid_c)
    normed_own = (resid_c * scale_c * gains[2]).astype(bf16)
    branch = (attn_out + cross_res).astype(bf16)

    normed_half = lax.dynamic_slice_in_dim(normed_own, core * half, half, 0)
    normed_other = halves(to_peer(normed_half))

    def forward(normed):
        gate_pre = project(ffn_in[0], normed)
        up_pre = project(ffn_in[1], normed)
        hidden = gated_unit(gate_pre, up_pre).astype(bf16)
        return gate_pre, up_pre, hidden, project(ffn_out, hidden)

    def backward(gate_pre, up_pre, grad_rows):
        grad_hidden = dot_nn(ffn_out, grad_rows)
        _, gate_back = jax.vjp(gated_unit, gate_pre, up_pre)
        grad_gate, grad_up = (g.astype(bf16) for g in gate_back(grad_hidden))
        back = dot_nn(ffn_in[0], grad_gate) + dot_nn(ffn_in[1], grad_up)
        return grad_gate, grad_up, back

    def my_half(part):
        split = part.reshape(2, 2, depth, length)
        got = to_mate(pick(split, 1 - core, 1).astype(bf16))
        return pick(split, core, 1) + got.astype(f32)

    block = width // dp_size

    place = lax.axis_index(DP)
    outer, inner = place // 2, place % 2
    count = dp_size // 2

    def dp_start(mats):
        split = mats.reshape(mats.shape[0], count, 2, *mats.shape[2:])
        swap = [(i, i ^ 1) for i in range(dp_size)]
        sent = pick(split, 1 - inner, 2)
        got = lax.ppermute(sent, DP, swap)
        return pick(split, inner, 2), sent, got

    def dp_terms(started):
        mine = (started[0].astype(f32) + started[2].astype(f32)).astype(bf16)
        terms = [pick(mine, outer, 1)]
        for o in [(count // 2 + i) % count for i in range(count)]:
            if o:
                turn = [(i, (i + 2 * o) % dp_size) for i in range(dp_size)]
                terms.append(lax.ppermute(pick(mine, (outer + o) % count, 1), DP, turn))
        return terms

    def near_far(inner):
        split = inner.reshape(4, depth, inner.shape[1])
        return pick(split, me), pick(split, far)

    gate_o, up_o, hid_o, res_o = forward(normed_own)
    gg_o, gu_o, back_o = backward(gate_o, up_o, grad_own)
    normed_other = after(normed_other, gg_o, gu_o, back_o)
    gate_t, up_t, hid_t, res_t = forward(normed_other)
    gg_t, gu_t, back_t = backward(gate_t, up_t, grad_other)

    grad_in = [
        (dot_nt(normed_own, own) + dot_nt(normed_other, other)).astype(bf16)
        for own, other in ((gg_o, gg_t), (gu_o, gu_t))
    ]
    grad_out = (dot_nt(grad_own, hid_o) + dot_nt(grad_other, hid_t)).astype(bf16)
    ffn_joined = jnp.stack(grad_in + [grad_out]).reshape(3, dp_size, block, width)
    back_sent = my_half(back_t).astype(bf16)
    back_far = to_peer(back_sent)
    sum_o = my_half(res_o) + pick(branch.reshape(2, 2, depth, length), core, 1).astype(f32)
    sum_t = my_half(res_t)
    sum_sent = jnp.stack([pick(sum_o, 1 - chip), pick(sum_t, 1 - chip)]).astype(bf16)
    ffn_started = dp_start(ffn_joined)
    enc_near_far = near_far(enc.T)
    back_far, sum_sent, enc_near_far, _ = lax.optimization_barrier(
        (back_far, sum_sent, enc_near_far, ffn_started[1])
    )
    back_half = my_half(back_o) + back_far.astype(f32)
    back_mate = to_mate(back_half.astype(bf16)).astype(f32)
    back_both = jnp.stack([back_half, back_mate])
    grad_normed_c = jnp.stack([pick(back_both, core), pick(back_both, 1 - core)], axis=1).reshape(
        width, length
    )

    ffn_terms = dp_terms(ffn_started)

    sum_far = to_peer(sum_sent)


    def rms_back(values, scale, gain, incoming):
        inner = jnp.mean(gain * incoming * values, axis=0, keepdims=True)
        return (
            scale * gain * incoming - values * (scale * scale * scale) * inner,
            jnp.sum(incoming * values * scale, axis=1),
        )

    grad_rows = grad_own.astype(f32)
    grad_resid_c, gain_grad_c = rms_back(resid_c, scale_c, gains[2], grad_normed_c)
    grad_cross_b = (grad_rows + grad_resid_c).astype(bf16)
    cross_out_rows = lax.dynamic_slice_in_dim(w_cross_out, core * half, half, 0)
    grad_cmix = dot_nn(cross_out_rows, grad_cross_b).astype(bf16)
    gcq, gck, gcv = attention_call(*cross_args, (cross_log, cmix_own, grad_cmix), 512)
    gcq_all, gck_all, gcv_all = halves(gcq), halves(gck), halves(gcv)
    grad_normed_b = dot_nn(w_cross[0], gcq_all)
    side_keep, side_send = outer_products(
        (
            ((gcq_all,), near_far(normed_b)),
            ((gck_all, gcv_all), enc_near_far),
            ((grad_cross_b,), near_far(cross_mix)),
        )
    )
    side_got = to_peer(side_send)
    enc_rows = encoder.shape[1]

    def encoder_grad(which):
        keys = lax.dynamic_slice_in_dim(gck_all, which * enc_rows, enc_rows, 1)
        values = lax.dynamic_slice_in_dim(gcv_all, which * enc_rows, enc_rows, 1)
        return dot_tt(keys, w_cross[1]) + dot_tt(values, w_cross[2])

    enc_got = to_peer(encoder_grad(far).astype(bf16))

    resid_b_part, gain_grad_b = rms_back(resid_b, scale_b, gains[1], grad_normed_b)
    grad_resid_b = grad_resid_c + resid_b_part
    grad_attn_b = (grad_rows + grad_resid_b).astype(bf16)
    self_out_rows = lax.dynamic_slice_in_dim(w_self_out, core * half, half, 0)
    grad_mix = dot_nn(self_out_rows, grad_attn_b).astype(bf16)
    g_own = attention_call(*self_args, (self_log, mix_own, grad_mix), 256)
    g_mate = [to_mate(g) for g in g_own]
    mix_near, mix_far = near_far(self_mix)
    attn_halves = grad_attn_b.reshape(2, half, length)
    where = core.astype(jnp.int32).reshape(1)
    grads = (*g_own, *g_mate)
    send = self_products(grads, normed_pieces[1], attn_halves, mix_far, where)
    sum_far, enc_got, send = lax.optimization_barrier((sum_far, enc_got, send))
    side_sum = (side_keep.astype(f32) + side_got.astype(f32)).astype(bf16)
    side_started = dp_start(side_sum.reshape(2, dp_size, block, 2 * depth))
    branch_sum = by_row(
        pick(sum_o, chip) + sum_far[1].astype(f32), pick(sum_t, chip) + sum_far[0].astype(f32)
    )
    new_state = jnp.stack(
        [guess_a + correct[0] * branch_sum, guess_b + correct[1] * branch_sum], axis=1
    ).astype(bf16)
    grad_correct = (jnp.sum(cot_a * branch_sum), jnp.sum(cot_b * branch_sum))
    grad_encoder = by_row(encoder_grad(me), enc_got.astype(f32))
    got = to_peer(send)
    keep = self_products(grads, normed_pieces[0], attn_halves, mix_near, where)
    both_in = into_active(grads, (own_near, mate_near, own_far, mate_far))
    blocks = (2, 2, count, block, 2 * depth)
    side_terms = dp_terms(side_started)
    finished = finish(keep.reshape(blocks), got.reshape(blocks), side_terms, ffn_terms, dp_size)
    both_act = jnp.stack([act_own, act_far]).astype(f32)
    gain_a = norm_gains[0].reshape(4, depth)
    both_gain = jnp.stack([pick(gain_a, me), pick(gain_a, far)])[:, :, None]
    inner = jnp.sum(both_gain * both_in * both_act, axis=(0, 1))[None]
    inner = (inner + to_mate(inner)) / width
    split_b = grad_resid_b.reshape(4, depth, length)
    both_b = jnp.stack([pick(split_b, me), pick(split_b, far)])
    both_back = scale_a * both_gain * both_in - both_act * (scale_a * scale_a * scale_a) * inner
    grad_active = (both_b + both_back).astype(bf16)
    gain_sums = jnp.sum(both_in * both_act * scale_a, axis=2)
    slot = jnp.arange(4, dtype=jnp.int32)[:, None]
    gain_grad_a = (
        jnp.where(slot == me, gain_sums[0][None], 0.0)
        + jnp.where(slot == far, gain_sums[1][None], 0.0)
    ).reshape(width)

    active_got = to_peer(grad_active[1])
    grad_state, late_sums = state_grads(
        predict, chip.astype(jnp.int32).reshape(1), wide_state, cotangent, grad_active[0], active_got
    )
    early = (*early_sums, *grad_correct)
    gain_sums = jnp.stack([gain_grad_a, 0.5 * gain_grad_b, 0.5 * gain_grad_c])
    total = all_sum(early, late_sums, gain_sums, dp_size, 4)

    return (
        new_state,
        grad_state,
        grad_encoder,
        *finished,
        total[:3],
        total[3, :4].reshape(2, 2),
        total[3, 4:6],
    )


def choose(paired, dp_size, wide_state, *rest):
    if paired and wide_state.shape[0] == 2:
        return paired_shards(dp_size, wide_state, *rest)
    return shards(wide_state, *rest)


def solution(mesh):
    in_specs = (
        P("dp", None, "mp", None),
        P("dp", "mp", None),
        P("dp", None),
        P("dp", None),
        P(None, "mp", None),
        P("mp", None),
        P(None, "mp", None),
        P("mp", None),
        P(None, None, "mp"),
        P("mp", None),
        P(),
        P(),
        P(),
        P("dp", None, "mp", None),
    )
    out_specs = (
        P("dp", None, "mp", None),
        P("dp", None, "mp", None),
        P("dp", "mp", None),
        P(None, "mp", "dp"),
        P("mp", "dp"),
        P(None, "mp", "dp"),
        P("mp", "dp"),
        P(None, "dp", "mp"),
        P("mp", "dp"),
        P(),
        P(),
        P(),
    )
    paired = mesh.shape["mp"] == 4
    body = functools.partial(choose, paired, mesh.shape["dp"])
    return jax.shard_map(
        body, mesh=mesh, in_specs=in_specs, out_specs=out_specs, check_vma=False
    )
```
